128 devices in a mesh: dp: 1, ctx: 128 (over z, y, x, core).
Axes of the slice: x: 4, y: 4, z: 4, core: 2. Of those that a mesh axis runs over, the one named last changes fastest.
Arguments:
- q_seq: bfloat16 [1, 32768, 4, 128], P('dp', 'ctx')
- k_seq: bfloat16 [1, 32768, 1, 128], P('dp', 'ctx')
- v_seq: bfloat16 [1, 32768, 1, 128], P('dp', 'ctx')
- do_seq: bfloat16 [1, 32768, 4, 128], P('dp', 'ctx')
Outputs:
- output 1: bfloat16 [1, 32768, 4, 128], P('dp', 'ctx')
- output 2: bfloat16 [1, 32768, 4, 128], P('dp', 'ctx')
- output 3: bfloat16 [1, 32768, 1, 128], P('dp', 'ctx')
- output 4: bfloat16 [1, 32768, 1, 128], P('dp', 'ctx')
All inputs are finite; a program needn't handle non-finite values.
Results may differ from the reference program's by a relative error of at most 0.00819087.
Values are sent between devices in bfloat16 or wider.
A program may use at most 1 GiB of HBM per device.

```python
import math
import jax
import jax.numpy as jnp
from jax import lax

BATCH = 1
CTX = 128
CHUNK = 256
Q_HEADS = 4
KV_LOCAL = 1
HEAD = 128
WINDOW = 4096

SEQ = CTX * CHUNK
GROUP = Q_HEADS // KV_LOCAL
QBLK = min(CHUNK, 128)
NEG_BIG = -1e30


def setup_inputs(seed: int = 0, part: int = 0) -> dict:
    base_key = jax.random.fold_in(jax.random.key(seed), part)
    key_q, key_k, key_v, key_do = jax.random.split(base_key, 4)
    input_std = (0.5 * math.log(WINDOW)) ** 0.25
    q_shape = (BATCH, SEQ, Q_HEADS, HEAD)
    kv_shape = (BATCH, SEQ, KV_LOCAL, HEAD)
    q_seq = input_std * jax.random.normal(key_q, q_shape, jnp.float32)
    k_seq = input_std * jax.random.normal(key_k, kv_shape, jnp.float32)
    v_seq = jax.random.normal(key_v, kv_shape, jnp.float32)
    do_seq = jax.random.normal(key_do, q_shape, jnp.float32)
    return {'q_seq': q_seq.astype(jnp.bfloat16), 'k_seq': k_seq.astype(jnp.bfloat16), 'v_seq': v_seq.astype(jnp.bfloat16), 'do_seq': do_seq.astype(jnp.bfloat16)}


def attend_all(q_full, k_full, v_full):
    n_blk = SEQ // QBLK
    q_blocks = jnp.moveaxis(q_full.reshape(BATCH, n_blk, QBLK, KV_LOCAL, GROUP, HEAD), 1, 0)
    pad_width = ((0, 0), (WINDOW, 0), (0, 0), (0, 0))
    k_pad = jnp.pad(k_full, pad_width)
    v_pad = jnp.pad(v_full, pad_width)
    span_len = WINDOW + QBLK
    dist = jnp.arange(QBLK)[:, None] + WINDOW - jnp.arange(span_len)[None, :]
    pair_ok = (dist >= 0) & (dist < WINDOW)
    sm_scale = HEAD ** -0.5

    def one_block(blk_args):
        blk_id, q_blk = blk_args
        start = blk_id * QBLK
        k_win = lax.dynamic_slice_in_dim(k_pad, start, span_len, axis=1)
        v_win = lax.dynamic_slice_in_dim(v_pad, start, span_len, axis=1)
        keep_mask = pair_ok & (jnp.arange(span_len)[None, :] + start >= WINDOW)
        scores = jnp.einsum('bqhgd,bkhd->bhgqk', q_blk, k_win) * sm_scale
        scores = jnp.where(keep_mask, scores, NEG_BIG)
        weights = jax.nn.softmax(scores, axis=-1)
        return jnp.einsum('bhgqk,bkhd->bqhgd', weights, v_win)

    o_blocks = lax.map(jax.checkpoint(one_block), (jnp.arange(n_blk), q_blocks))
    return jnp.moveaxis(o_blocks, 0, 1).reshape(BATCH, SEQ, Q_HEADS, HEAD)


def reference(q_seq, k_seq, v_seq, do_seq):
    o_full, pull_back = jax.vjp(attend_all, q_seq.astype(jnp.float32), k_seq.astype(jnp.float32), v_seq.astype(jnp.float32))
    dq_full, dk_full, dv_full = pull_back(do_seq.astype(jnp.float32))
    return (o_full.astype(jnp.bfloat16), dq_full.astype(jnp.bfloat16), dk_full.astype(jnp.bfloat16), dv_full.astype(jnp.bfloat16))
```

```python
import functools

import jax
import jax.numpy as jnp
from jax import lax
from jax.experimental import pallas as pl
from jax.experimental.pallas import tpu as pltpu
from jax.sharding import PartitionSpec as P

OWN, Y1, AT, AO, A2, BT, BO, B2, Y2 = 0, 1, 3, 4, 7, 9, 10, 13, 16
PY1, PAT, PAO, PA2, PBT, PBO, PB2, PS = 2, 5, 6, 8, 11, 12, 14, 15
N_SLOT = 17
ROW = 8
N_DEV = 128
CH = 256
NQ = 1024
HD = 128
TILE = 256
NEG_BIG = -1e30
LOG2E = 1.4426950408889634
SCALE = HD ** -0.5
F32 = jnp.float32
BF16 = jnp.bfloat16


def dot(a, b):
    return lax.dot_general(a, b, (((1,), (0,)), ((), ())), preferred_element_type=F32)


def kernel(q_hbm, k_hbm, v_hbm, do_hbm, o_hbm, dq_hbm, dk_hbm, dv_hbm,
           kv, q_s, do_s, qt_s, dot_s, p_buf, dp_buf, mh, m_s, l_s, d_s, ot_s, dqt_s, part,
           dr, rx, o_s, dq_s, dkv_s,
           lsem, fs, fr, bs, br):
    me = lax.axis_index('ctx')
    core = lax.rem(me, 2)
    x = lax.rem(lax.div(me, 2), 4)
    odd = lax.rem(x, 2)
    base = me - 2 * x
    x_left = lax.rem(x + 3, 4)
    x_right = lax.rem(x + 1, 4)
    x_f = x_left + odd * (x_right - x_left)
    x_g = x_right + odd * (x_left - x_right)
    x_2 = lax.rem(x + 2, 4)
    dev_f = base + 2 * x_f
    dev_g = base + 2 * x_g
    partner = me + 1 - 2 * core
    up = lax.rem(me + ROW, N_DEV)
    down = lax.rem(me + N_DEV - ROW, N_DEV)

    def dev(d):
        return {'dp': 0, 'ctx': d}

    loads = [
        pltpu.make_async_copy(k_hbm, kv.at[OWN, 0], lsem.at[0]),
        pltpu.make_async_copy(v_hbm, kv.at[OWN, 1], lsem.at[1]),
        pltpu.make_async_copy(q_hbm, q_s, lsem.at[2]),
        pltpu.make_async_copy(do_hbm, do_s, lsem.at[3]),
    ]
    for c in loads:
        c.start()

    barrier = pltpu.get_barrier_semaphore()
    peers = (partner, dev_f, dev_g, up, down)
    for d in peers:
        pl.semaphore_signal(barrier, inc=1, device_id=dev(d), device_id_type=pl.DeviceIdType.MESH)
    pl.semaphore_wait(barrier, len(peers))

    def kv_copy(msg, src, dst, d, j):
        return pltpu.make_async_remote_copy(
            src_ref=kv.at[src, j], dst_ref=kv.at[dst, j], send_sem=fs.at[msg, j], recv_sem=fr.at[dst, j],
            device_id=dev(d), device_id_type=pl.DeviceIdType.MESH)

    def kv_wait(slot, j):
        kv_copy(0, slot, slot, partner, j).wait_recv()

    def kv_send(msg, src, dst, d):
        for j in range(2):
            kv_copy(msg, src, dst, d, j).start()

    M_Y1, M_Y2, M_AT, M_AO, M_A2, M_BT, M_BO, M_B2 = range(8)
    M_P = {PY1: 8, PAT: 9, PAO: 10, PA2: 11, PBT: 12, PBO: 13, PB2: 14, PS: 15}

    def to_partner(src, dst):
        kv_send(M_P[dst], src, dst, partner)

    loads[0].wait()
    loads[1].wait()
    kv_send(M_Y1, OWN, Y1, up)

    @pl.when(x_g > x)
    def _():
        kv_send(M_BT, OWN, BT, dev_g)

    @pl.when(x_f > x)
    def _():
        kv_send(M_BO, OWN, BO, dev_f)

    @pl.when(core == 0)
    def _():
        to_partner(OWN, PS)

    loads[2].wait()
    loads[3].wait()
    for t in range(NQ // TILE):
        rows = pl.ds(t * TILE, TILE)
        qt_s[:, rows] = q_s[rows, :].T
        dot_s[:, rows] = do_s[rows, :].T
    m_s[...] = jnp.full_like(m_s, NEG_BIG)
    l_s[...] = jnp.zeros_like(l_s)
    ot_s[...] = jnp.zeros_like(ot_s)
    dqt_s[...] = jnp.zeros_like(dqt_s)

    def fwd_compute(slot, step_id, kind):
        kb = kv[slot, 0]
        vb = kv[slot, 1]
        vt = vb.T
        valid = me >= step_id
        hide = jnp.where(valid, 0.0, -NEG_BIG).astype(F32)
        for t in range(NQ // TILE):
            ls = pl.ds(t * TILE, TILE)
            s = dot(kb, qt_s[:, ls])
            if kind is not None:
                key = lax.broadcasted_iota(jnp.int32, (CH, TILE), 0)
                tok = lax.shift_right_logical(lax.broadcasted_iota(jnp.int32, (CH, TILE), 1) + t * TILE, 2)
                keep = key <= tok if kind == 'own' else key > tok
                s = jnp.where(keep, s, NEG_BIG)
            cm = jnp.max(s, axis=0, keepdims=True) * (SCALE * LOG2E)
            m_old = m_s[:, ls]
            m_new = jnp.maximum(m_old, cm - hide)
            p = jnp.exp2(s * (SCALE * LOG2E) - (m_new + hide))
            p_buf[slot, :, ls] = p
            alpha = jnp.exp2(m_old - m_new)
            m_s[:, ls] = m_new
            mh[slot, :, ls] = m_new
            l_s[:, ls] = l_s[:, ls] * alpha + jnp.sum(p, axis=0, keepdims=True)
            ot_s[:, ls] = ot_s[:, ls] * alpha + dot(vt, p.astype(BF16))
            dp_buf[slot, :, ls] = dot(vb, dot_s[:, ls])

    fwd_compute(OWN, 0, 'own')

    d_f, d_g, d_2 = x - x_f, x - x_g, x - x_2

    def wrap8(d):
        return d + 8 * (d < 0).astype(jnp.int32)

    def chip_dist(i):
        table = {Y1: 4, PY1: 4, AT: 4 + d_f, AO: 4 + d_g, PAT: 4 + d_f, PAO: 4 + d_g, A2: 4 + d_2, PA2: 4 + d_2,
                 BT: wrap8(d_g), BO: wrap8(d_f), PBT: wrap8(d_g), PBO: wrap8(d_f), B2: wrap8(d_2), PB2: wrap8(d_2),
                 PS: 8 * (1 - core)}
        d = 0
        for slot, dist in table.items():
            d = d + (i == slot).astype(jnp.int32) * dist
        return d

    def is_partner(i):
        f = 0
        for slot in M_P:
            f = f + (i == slot).astype(jnp.int32)
        return f

    def fwd_body(i, carry):
        kv_wait(i, 0)
        kv_wait(i, 1)

        @pl.when(i == Y1)
        def _():
            kv_send(M_Y2, Y1, Y2, up)
            kv_send(M_AT, Y1, AT, dev_f)
            kv_send(M_AO, Y1, AO, dev_g)
            to_partner(Y1, PY1)

        @pl.when(i == AT)
        def _():
            to_partner(AT, PAT)

        @pl.when(i == AO)
        def _():
            kv_send(M_A2, AO, A2, dev_f)
            to_partner(AO, PAO)
            kv_wait(Y2, 0)
            kv_wait(Y2, 1)

            @pl.when(x_g < x)
            def _():
                kv_send(M_BT, Y2, BT, dev_g)

            @pl.when(x_f < x)
            def _():
                kv_send(M_BO, Y2, BO, dev_f)

            @pl.when(core == 1)
            def _():
                to_partner(Y2, PS)

        @pl.when(i == A2)
        def _():
            to_partner(A2, PA2)

        @pl.when(i == BT)
        def _():
            to_partner(BT, PBT)

        @pl.when(i == BO)
        def _():
            kv_send(M_B2, BO, B2, dev_g)
            to_partner(BO, PBO)

        @pl.when(i == B2)
        def _():
            to_partner(B2, PB2)

        step_id = 2 * chip_dist(i) + is_partner(i) * (2 * core - 1)
        fwd_compute(i, step_id, None)
        return carry

    lax.fori_loop(1, N_SLOT - 1, fwd_body, 0)
    fwd_compute(Y2, 16, 'far')

    for t in range(NQ // TILE):
        ls = pl.ds(t * TILE, TILE)
        rl = 1.0 / l_s[:, ls]
        l_s[:, ls] = rl
        ot = ot_s[:, ls] * rl
        d_s[:, ls] = jnp.sum(ot * dot_s[:, ls].astype(F32), axis=0, keepdims=True)
        o_s[ls, :] = ot.T.astype(BF16)
    o_out = pltpu.make_async_copy(o_s, o_hbm, lsem.at[4])
    o_out.start()

    def part_copy(msg, src, dst_ref, d, j, sem):
        return pltpu.make_async_remote_copy(
            src_ref=part.at[src, j], dst_ref=dst_ref, send_sem=bs.at[msg, j], recv_sem=br.at[sem, j],
            device_id=dev(d), device_id_type=pl.DeviceIdType.MESH)

    R_A2, R_B2, R_AT, R_AO, R_BT, R_BO, R_Y2, R_YA = range(8)

    def give(src, n):
        for j in (1, 0):
            part_copy(n, src, dr.at[n, j], partner, j, n).start()

    def got(n, j):
        part_copy(n, 0, dr.at[n, j], partner, j, n).wait_recv()

    def send(src, n, d, j):
        part_copy(8 + n, src, rx.at[n, j], d, j, 8 + n).start()

    def recv(n, j):
        part_copy(8 + n, 0, rx.at[n, j], partner, j, 8 + n).wait_recv()

    D_SLOT = {PY1: 0, PAT: 1, PAO: 2, PA2: 3, PBT: 4, PBO: 5, PB2: 6, PS: 7}

    def merge_send(slot, n_d, n_r, d):
        for j in (1, 0):
            got(n_d, j)
            part[slot, j] += dr[n_d, j]
            send(slot, n_r, d, j)

    def bwd_body(t0, carry):
        i = N_SLOT - 1 - t0
        kb = kv[i, 0]
        kt = kb.T
        dk = jnp.zeros((CH, HD), F32)
        dv = jnp.zeros((CH, HD), F32)
        for t in range(NQ // TILE):
            ls = pl.ds(t * TILE, TILE)
            f = jnp.exp2(mh[i, :, ls] - m_s[:, ls]) * l_s[:, ls]
            p = p_buf[i, :, ls] * f
            dv = dv + dot(p.astype(BF16), do_s[ls, :])
            ds = (p * (dp_buf[i, :, ls] - d_s[:, ls])).astype(BF16)
            dk = dk + dot(ds, q_s[ls, :])
            dqt_s[:, ls] += dot(kt, ds)
        part[i, 0] = dk * SCALE
        part[i, 1] = dv

        for slot, n in D_SLOT.items():
            @pl.when(i == slot)
            def _(slot=slot, n=n):
                give(slot, n)

        @pl.when(i == B2)
        def _():
            merge_send(B2, 6, R_B2, dev_g)

        @pl.when(i == BT)
        def _():
            merge_send(BT, 4, R_BT, dev_g)

        @pl.when(i == A2)
        def _():
            merge_send(A2, 3, R_A2, dev_f)

        @pl.when(i == AT)
        def _():
            merge_send(AT, 1, R_AT, dev_f)

        return carry

    lax.fori_loop(0, N_SLOT, bwd_body, 0)

    def relay(slot, n_d, n_in, n_out, d):
        for j in (1, 0):
            got(n_d, j)
            recv(n_in, j)
            part[slot, j] += dr[n_d, j] + rx[n_in, j]
            send(slot, n_out, d, j)

    relay(BO, 5, R_B2, R_BO, dev_f)
    relay(AO, 2, R_A2, R_AO, dev_g)

    for t in range(NQ // TILE):
        ls = pl.ds(t * TILE, TILE)
        dq_s[ls, :] = (dqt_s[:, ls] * SCALE).T.astype(BF16)
    dq_out = pltpu.make_async_copy(dq_s, dq_hbm, lsem.at[5])
    dq_out.start()

    def home_or_far(far):
        return far.astype(jnp.int32) * Y2

    for j in (1, 0):
        got(0, j)
        part[Y1, j] += dr[0, j]
        got(7, j)
        part[core * Y2, j] += dr[7, j]
    for j in (1, 0):
        recv(R_BT, j)
        part[home_or_far(x_g < x), j] += rx[R_BT, j]
        recv(R_BO, j)
        part[home_or_far(x_f < x), j] += rx[R_BO, j]
        send(Y2, R_Y2, down, j)
    for j in (1, 0):
        recv(R_AT, j)
        recv(R_AO, j)
        part[Y1, j] += rx[R_AT, j] + rx[R_AO, j]
    for j in (1, 0):
        recv(R_Y2, j)
        part[Y1, j] += rx[R_Y2, j]
        send(Y1, R_YA, down, j)
    outs = []
    for j, hbm in ((1, dv_hbm), (0, dk_hbm)):
        recv(R_YA, j)
        dkv_s[j] = (part[OWN, j] + rx[R_YA, j]).astype(BF16)
        c = pltpu.make_async_copy(dkv_s.at[j], hbm, lsem.at[6 + j])
        c.start()
        outs.append(c)

    for msg in range(16):
        for j in range(2):
            kv_copy(msg, 0, 0, partner, j).wait_send()
            part_copy(msg, 0, dr.at[0, j], partner, j, 0).wait_send()
    o_out.wait()
    dq_out.wait()
    for c in outs:
        c.wait()


def solution(mesh):
    seq_spec = P('dp', 'ctx', None, None)

    def local_attn(q_loc, k_loc, v_loc, do_loc):
        q = q_loc.reshape(NQ, HD)
        do = do_loc.reshape(NQ, HD)
        k = k_loc.reshape(CH, HD)
        v = v_loc.reshape(CH, HD)
        anyspec = pl.BlockSpec(memory_space=pl.ANY)
        o, dq, dk, dv = pl.pallas_call(
            kernel,
            out_shape=(jax.ShapeDtypeStruct((NQ, HD), BF16), jax.ShapeDtypeStruct((NQ, HD), BF16),
                       jax.ShapeDtypeStruct((CH, HD), BF16), jax.ShapeDtypeStruct((CH, HD), BF16)),
            in_specs=[anyspec] * 4,
            out_specs=[anyspec] * 4,
            scratch_shapes=[
                pltpu.VMEM((N_SLOT, 2, CH, HD), BF16),
                pltpu.VMEM((NQ, HD), BF16),
                pltpu.VMEM((NQ, HD), BF16),
                pltpu.VMEM((HD, NQ), BF16),
                pltpu.VMEM((HD, NQ), BF16),
                pltpu.VMEM((N_SLOT, CH, NQ), F32),
                pltpu.VMEM((N_SLOT, CH, NQ), F32),
                pltpu.VMEM((N_SLOT, 1, NQ), F32),
                pltpu.VMEM((1, NQ), F32),
                pltpu.VMEM((1, NQ), F32),
                pltpu.VMEM((1, NQ), F32),
                pltpu.VMEM((HD, NQ), F32),
                pltpu.VMEM((HD, NQ), F32),
                pltpu.VMEM((N_SLOT, 2, CH, HD), F32),
                pltpu.VMEM((8, 2, CH, HD), F32),
                pltpu.VMEM((8, 2, CH, HD), F32),
                pltpu.VMEM((NQ, HD), BF16),
                pltpu.VMEM((NQ, HD), BF16),
                pltpu.VMEM((2, CH, HD), BF16),
                pltpu.SemaphoreType.DMA((8,)),
                pltpu.SemaphoreType.DMA((16, 2)),
                pltpu.SemaphoreType.DMA((N_SLOT, 2)),
                pltpu.SemaphoreType.DMA((16, 2)),
                pltpu.SemaphoreType.DMA((16, 2)),
            ],
            compiler_params=pltpu.CompilerParams(
                collective_id=0, has_side_effects=True, vmem_limit_bytes=63 * 1024 * 1024),
            name='swa_fwd_bwd',
        )(q, k, v, do)
        return o.reshape(q_loc.shape), dq.reshape(q_loc.shape), dk.reshape(k_loc.shape), dv.reshape(k_loc.shape)

    return jax.shard_map(local_attn, mesh=mesh, in_specs=(seq_spec,) * 4, out_specs=(seq_spec,) * 4, check_vma=False)
```

```python
import functools

import jax
import jax.numpy as jnp
from jax import lax
from jax.experimental import pallas as pl
from jax.experimental.pallas import tpu as pltpu
from jax.sharding import PartitionSpec as P

OWN, Y1, AT, AO, A2, BT, BO, B2, Y2 = 0, 1, 3, 4, 7, 9, 10, 13, 16
PY1, PAT, PAO, PA2, PBT, PBO, PB2, PS = 2, 5, 6, 8, 11, 12, 14, 15
N_SLOT = 17
ROW = 8
N_DEV = 128
CH = 256
NQ = 1024
HD = 128
TILE = 256
NEG_BIG = -1e30
LOG2E = 1.4426950408889634
SCALE = HD ** -0.5
F32 = jnp.float32
BF16 = jnp.bfloat16


def dot(a, b):
    return lax.dot_general(a, b, (((1,), (0,)), ((), ())), preferred_element_type=F32)


def kernel(q_hbm, k_hbm, v_hbm, do_hbm, o_hbm, dq_hbm, dk_hbm, dv_hbm,
           kv, q_s, do_s, qt_s, dot_s, p_buf, dp_buf, mh, m_s, l_s, d_s, ot_s, dqt_s, part,
           dr, rx, o_s, dq_s, dkv_s,
           lsem, fs, fr, bs, br):
    me = lax.axis_index('ctx')
    core = lax.rem(me, 2)
    x = lax.rem(lax.div(me, 2), 4)
    odd = lax.rem(x, 2)
    base = me - 2 * x
    x_left = lax.rem(x + 3, 4)
    x_right = lax.rem(x + 1, 4)
    x_f = x_left + odd * (x_right - x_left)
    x_g = x_right + odd * (x_left - x_right)
    x_2 = lax.rem(x + 2, 4)
    dev_f = base + 2 * x_f
    dev_g = base + 2 * x_g
    partner = me + 1 - 2 * core
    up = lax.rem(me + ROW, N_DEV)
    down = lax.rem(me + N_DEV - ROW, N_DEV)

    def dev(d):
        return {'dp': 0, 'ctx': d}

    loads = [
        pltpu.make_async_copy(k_hbm, kv.at[OWN, 0], lsem.at[0]),
        pltpu.make_async_copy(v_hbm, kv.at[OWN, 1], lsem.at[1]),
        pltpu.make_async_copy(q_hbm, q_s, lsem.at[2]),
        pltpu.make_async_copy(do_hbm, do_s, lsem.at[3]),
    ]
    for c in loads:
        c.start()

    row = lax.div(me, ROW)
    has_up = row < N_DEV // ROW - 1
    e1 = row >= 1
    e2 = row >= 2
    e_bt = jnp.logical_or(x_g < x, e2)
    e_bo = jnp.logical_or(x_f < x, e2)
    e_b2 = jnp.logical_or(x_2 < x, e2)

    barrier = pltpu.get_barrier_semaphore()

    def greet(d):
        pl.semaphore_signal(barrier, inc=1, device_id=dev(d), device_id_type=pl.DeviceIdType.MESH)

    pl.when(has_up)(lambda: greet(up))
    pl.when(e1)(lambda: greet(down))
    for d in (dev_f, dev_g, partner):
        greet(d)
    pl.semaphore_wait(barrier, 3 + has_up.astype(jnp.int32) + e1.astype(jnp.int32))

    def kv_copy(msg, src, dst, d, j):
        return pltpu.make_async_remote_copy(
            src_ref=kv.at[src, j], dst_ref=kv.at[dst, j], send_sem=fs.at[msg, j], recv_sem=fr.at[dst, j],
            device_id=dev(d), device_id_type=pl.DeviceIdType.MESH)

    def kv_wait(slot, j):
        kv_copy(0, slot, slot, partner, j).wait_recv()

    def kv_send(msg, src, dst, d, j):
        kv_copy(msg, src, dst, d, j).start()

    M_Y1, M_Y2, M_AT, M_AO, M_A2, M_BT, M_BO, M_B2 = range(8)
    M_P = {PY1: 8, PAT: 9, PAO: 10, PA2: 11, PBT: 12, PBO: 13, PB2: 14, PS: 15}

    def to_partner(src, dst, j):
        kv_send(M_P[dst], src, dst, partner, j)

    for j in range(2):
        loads[j].wait()
        pl.when(has_up)(lambda: kv_send(M_Y1, OWN, Y1, up, j))
        pl.when(x_g > x)(lambda: kv_send(M_BT, OWN, BT, dev_g, j))
        pl.when(x_f > x)(lambda: kv_send(M_BO, OWN, BO, dev_f, j))
        pl.when(core == 0)(lambda: to_partner(OWN, PS, j))

    loads[2].wait()
    loads[3].wait()
    for t in range(NQ // TILE):
        rows = pl.ds(t * TILE, TILE)
        qt_s[:, rows] = q_s[rows, :].T
        dot_s[:, rows] = do_s[rows, :].T
    m_s[...] = jnp.full_like(m_s, NEG_BIG)
    l_s[...] = jnp.zeros_like(l_s)
    ot_s[...] = jnp.zeros_like(ot_s)
    dqt_s[...] = jnp.zeros_like(dqt_s)

    def fwd_compute(slot, kind):
        kb = kv[slot, 0]
        vb = kv[slot, 1]
        vt = vb.T
        for t in range(NQ // TILE):
            ls = pl.ds(t * TILE, TILE)
            s = dot(kb, qt_s[:, ls])
            if kind is not None:
                key = lax.broadcasted_iota(jnp.int32, (CH, TILE), 0)
                tok = lax.shift_right_logical(lax.broadcasted_iota(jnp.int32, (CH, TILE), 1) + t * TILE, 2)
                keep = key <= tok if kind == 'own' else key > tok
                s = jnp.where(keep, s, NEG_BIG)
            cm = jnp.max(s, axis=0, keepdims=True) * (SCALE * LOG2E)
            m_old = m_s[:, ls]
            m_new = jnp.maximum(m_old, cm)
            p = jnp.exp2(s * (SCALE * LOG2E) - m_new)
            p_buf[slot, :, ls] = p
            alpha = jnp.exp2(m_old - m_new)
            m_s[:, ls] = m_new
            mh[slot, :, ls] = m_new
            l_s[:, ls] = l_s[:, ls] * alpha + jnp.sum(p, axis=0, keepdims=True)
            ot_s[:, ls] = ot_s[:, ls] * alpha + dot(vt, p.astype(BF16))
            dp_buf[slot, :, ls] = dot(vb, dot_s[:, ls])

    fwd_compute(OWN, 'own')

    def here(i):
        n = jnp.int32(0)
        for slots, e in (((Y1, PY1, AT, AO, PAT, PAO, A2, PA2), e1), ((BT, PBT), e_bt), ((BO, PBO), e_bo),
                         ((B2, PB2), e_b2), ((PS,), jnp.logical_or(core == 1, e2)), ((OWN,), row >= 0), ((Y2,), e2)):
            for slot in slots:
                n = n + (i == slot).astype(jnp.int32) * e.astype(jnp.int32)
        return n > 0

    def fwd_body(i, carry):
        @pl.when(here(i))
        def _():
            @pl.when(i == Y1)
            def _():
                for j in range(2):
                    kv_wait(Y1, j)
                    pl.when(has_up)(lambda: kv_send(M_Y2, Y1, Y2, up, j))
                    kv_send(M_AT, Y1, AT, dev_f, j)
                    kv_send(M_AO, Y1, AO, dev_g, j)
                    to_partner(Y1, PY1, j)

            @pl.when(i == AT)
            def _():
                for j in range(2):
                    kv_wait(AO, j)
                    kv_send(M_A2, AO, A2, dev_f, j)
                    to_partner(AO, PAO, j)

                    @pl.when(e2)
                    def _():
                        kv_wait(Y2, j)
                        pl.when(x_g < x)(lambda: kv_send(M_BT, Y2, BT, dev_g, j))
                        pl.when(x_f < x)(lambda: kv_send(M_BO, Y2, BO, dev_f, j))
                        pl.when(core == 1)(lambda: to_partner(Y2, PS, j))

                    kv_wait(AT, j)
                    to_partner(AT, PAT, j)

            is_p = jnp.int32(0)
            for slot in M_P:
                is_p = is_p + (i == slot).astype(jnp.int32)

            @pl.when(is_p > 0)
            def _():
                kv_wait(i, 0)
                kv_wait(i, 1)

            fwd_compute(i, None)

        @pl.when(i == PAO)
        def _():
            for j in range(2):
                @pl.when(e_bo)
                def _():
                    kv_wait(BO, j)
                    kv_send(M_B2, BO, B2, dev_g, j)
                    to_partner(BO, PBO, j)

                @pl.when(e1)
                def _():
                    kv_wait(A2, j)
                    to_partner(A2, PA2, j)

                @pl.when(e_bt)
                def _():
                    kv_wait(BT, j)
                    to_partner(BT, PBT, j)

        @pl.when(i == BO)
        def _():
            @pl.when(e_b2)
            def _():
                for j in range(2):
                    kv_wait(B2, j)
                    to_partner(B2, PB2, j)

        return carry

    lax.fori_loop(1, N_SLOT - 1, fwd_body, 0)
    pl.when(e2)(lambda: fwd_compute(Y2, 'far'))

    for t in range(NQ // TILE):
        ls = pl.ds(t * TILE, TILE)
        rl = 1.0 / l_s[:, ls]
        l_s[:, ls] = rl
        ot = ot_s[:, ls] * rl
        d_s[:, ls] = jnp.sum(ot * dot_s[:, ls].astype(F32), axis=0, keepdims=True)
        o_s[ls, :] = ot.T.astype(BF16)
    o_out = pltpu.make_async_copy(o_s, o_hbm, lsem.at[4])
    o_out.start()

    def part_copy(msg, src, dst_ref, d, j, sem):
        return pltpu.make_async_remote_copy(
            src_ref=part.at[src, j], dst_ref=dst_ref, send_sem=bs.at[msg, j], recv_sem=br.at[sem, j],
            device_id=dev(d), device_id_type=pl.DeviceIdType.MESH)

    R_A2, R_B2, R_AT, R_AO, R_BT, R_BO, R_Y2, R_YA = range(8)

    def give(src, n):
        for j in (1, 0):
            part_copy(n, src, dr.at[n, j], partner, j, n).start()

    def got(n, j):
        part_copy(n, 0, dr.at[n, j], partner, j, n).wait_recv()

    def send(src, n, d, j):
        part_copy(8 + n, src, rx.at[n, j], d, j, 8 + n).start()

    def recv(n, j):
        part_copy(8 + n, 0, rx.at[n, j], partner, j, 8 + n).wait_recv()

    D_SLOT = {PY1: 0, PAT: 1, PAO: 2, PA2: 3, PBT: 4, PBO: 5, PB2: 6, PS: 7}

    def merge_send(slot, n_d, n_r, d):
        for j in (1, 0):
            got(n_d, j)
            part[slot, j] += dr[n_d, j]
            send(slot, n_r, d, j)

    def bwd_compute(i):
        kb = kv[i, 0]
        kt = kb.T
        dk = jnp.zeros((CH, HD), F32)
        dv = jnp.zeros((CH, HD), F32)
        for t in range(NQ // TILE):
            ls = pl.ds(t * TILE, TILE)
            f = jnp.exp2(mh[i, :, ls] - m_s[:, ls]) * l_s[:, ls]
            p = p_buf[i, :, ls] * f
            dv = dv + dot(p.astype(BF16), do_s[ls, :])
            ds = (p * (dp_buf[i, :, ls] - d_s[:, ls])).astype(BF16)
            dk = dk + dot(ds, q_s[ls, :])
            dqt_s[:, ls] += dot(kt, ds)
        part[i, 0] = dk * SCALE
        part[i, 1] = dv

        for slot, n in D_SLOT.items():
            @pl.when(i == slot)
            def _(slot=slot, n=n):
                give(slot, n)

        @pl.when(i == B2)
        def _():
            merge_send(B2, 6, R_B2, dev_g)

        @pl.when(i == BT)
        def _():
            merge_send(BT, 4, R_BT, dev_g)

        @pl.when(i == A2)
        def _():
            merge_send(A2, 3, R_A2, dev_f)

        @pl.when(i == AT)
        def _():
            merge_send(AT, 1, R_AT, dev_f)

    def bwd_body(t0, carry):
        i = N_SLOT - 1 - t0
        pl.when(here(i))(lambda: bwd_compute(i))

        @pl.when(jnp.logical_and(i == AO, e_bo))
        def _():
            relay(BO, 5, R_B2, R_BO, dev_f)

        return carry

    def relay(slot, n_d, n_in, n_out, d):
        for j in (1, 0):
            got(n_d, j)
            recv(n_in, j)
            part[slot, j] += dr[n_d, j] + rx[n_in, j]
            send(slot, n_out, d, j)

    lax.fori_loop(0, N_SLOT, bwd_body, 0)
    pl.when(e1)(lambda: relay(AO, 2, R_A2, R_AO, dev_g))

    for t in range(NQ // TILE):
        ls = pl.ds(t * TILE, TILE)
        dq_s[ls, :] = (dqt_s[:, ls] * SCALE).T.astype(BF16)
    dq_out = pltpu.make_async_copy(dq_s, dq_hbm, lsem.at[5])
    dq_out.start()

    def home_or_far(far):
        return far.astype(jnp.int32) * Y2

    def add_rx(slot, n, j):
        recv(n, j)
        part[slot, j] += rx[n, j]

    r_bt = jnp.logical_or(x < x_g, e2)
    r_bo = jnp.logical_or(x < x_f, e2)
    r_ps = jnp.logical_or(core == 0, e2)
    r_y2 = jnp.logical_and(has_up, e1)
    for j in (1, 0):
        @pl.when(r_ps)
        def _():
            got(7, j)
            part[core * Y2, j] += dr[7, j]

        pl.when(r_bt)(lambda: add_rx(home_or_far(x_g < x), R_BT, j))
        pl.when(r_bo)(lambda: add_rx(home_or_far(x_f < x), R_BO, j))
        pl.when(e2)(lambda: send(Y2, R_Y2, down, j))
    for j in (1, 0):
        @pl.when(e1)
        def _():
            got(0, j)
            part[Y1, j] += dr[0, j]
            add_rx(Y1, R_AT, j)
            add_rx(Y1, R_AO, j)
            pl.when(has_up)(lambda: add_rx(Y1, R_Y2, j))
            send(Y1, R_YA, down, j)
    outs = []
    for j, hbm in ((1, dv_hbm), (0, dk_hbm)):
        pl.when(has_up)(lambda: add_rx(OWN, R_YA, j))
        dkv_s[j] = part[OWN, j].astype(BF16)
        c = pltpu.make_async_copy(dkv_s.at[j], hbm, lsem.at[6 + j])
        c.start()
        outs.append(c)

    up1 = jnp.logical_and(has_up, e1)
    kv_sent = ((M_Y1, has_up), (M_Y2, up1), (M_AT, e1), (M_AO, e1), (M_A2, e1),
               (M_BT, jnp.logical_or(x_g > x, e2)), (M_BO, jnp.logical_or(x_f > x, e2)), (M_B2, e_bo),
               (M_P[PY1], e1), (M_P[PAT], e1), (M_P[PAO], e1), (M_P[PA2], e1), (M_P[PBT], e_bt), (M_P[PBO], e_bo),
               (M_P[PB2], e_b2), (M_P[PS], r_ps))
    part_sent = ((0, e1), (1, e1), (2, e1), (3, e1), (4, e_bt), (5, e_bo), (6, e_b2), (7, jnp.logical_or(core == 1, e2)),
                 (8 + R_A2, e1), (8 + R_B2, e_b2), (8 + R_AT, e1), (8 + R_AO, e1), (8 + R_BT, e_bt), (8 + R_BO, e_bo),
                 (8 + R_Y2, e2), (8 + R_YA, e1))
    for j in range(2):
        for msg, e in kv_sent:
            pl.when(e)(lambda: kv_copy(msg, 0, 0, partner, j).wait_send())
        for msg, e in part_sent:
            pl.when(e)(lambda: part_copy(msg, 0, dr.at[0, j], partner, j, 0).wait_send())
    o_out.wait()
    dq_out.wait()
    for c in outs:
        c.wait()


def solution(mesh):
    seq_spec = P('dp', 'ctx', None, None)

    def local_attn(q_loc, k_loc, v_loc, do_loc):
        q = q_loc.reshape(NQ, HD)
        do = do_loc.reshape(NQ, HD)
        k = k_loc.reshape(CH, HD)
        v = v_loc.reshape(CH, HD)
        anyspec = pl.BlockSpec(memory_space=pl.ANY)
        o, dq, dk, dv = pl.pallas_call(
            kernel,
            out_shape=(jax.ShapeDtypeStruct((NQ, HD), BF16), jax.ShapeDtypeStruct((NQ, HD), BF16),
                       jax.ShapeDtypeStruct((CH, HD), BF16), jax.ShapeDtypeStruct((CH, HD), BF16)),
            in_specs=[anyspec] * 4,
            out_specs=[anyspec] * 4,
            scratch_shapes=[
                pltpu.VMEM((N_SLOT, 2, CH, HD), BF16),
                pltpu.VMEM((NQ, HD), BF16),
                pltpu.VMEM((NQ, HD), BF16),
                pltpu.VMEM((HD, NQ), BF16),
                pltpu.VMEM((HD, NQ), BF16),
                pltpu.VMEM((N_SLOT, CH, NQ), F32),
                pltpu.VMEM((N_SLOT, CH, NQ), F32),
                pltpu.VMEM((N_SLOT, 1, NQ), F32),
                pltpu.VMEM((1, NQ), F32),
                pltpu.VMEM((1, NQ), F32),
                pltpu.VMEM((1, NQ), F32),
                pltpu.VMEM((HD, NQ), F32),
                pltpu.VMEM((HD, NQ), F32),
                pltpu.VMEM((N_SLOT, 2, CH, HD), F32),
                pltpu.VMEM((8, 2, CH, HD), F32),
                pltpu.VMEM((8, 2, CH, HD), F32),
                pltpu.VMEM((NQ, HD), BF16),
                pltpu.VMEM((NQ, HD), BF16),
                pltpu.VMEM((2, CH, HD), BF16),
                pltpu.SemaphoreType.DMA((8,)),
                pltpu.SemaphoreType.DMA((16, 2)),
                pltpu.SemaphoreType.DMA((N_SLOT, 2)),
                pltpu.SemaphoreType.DMA((16, 2)),
                pltpu.SemaphoreType.DMA((16, 2)),
            ],
            compiler_params=pltpu.CompilerParams(
                collective_id=0, has_side_effects=True, vmem_limit_bytes=63 * 1024 * 1024),
            name='swa_fwd_bwd',
        )(q, k, v, do)
        return o.reshape(q_loc.shape), dq.reshape(q_loc.shape), dk.reshape(k_loc.shape), dv.reshape(k_loc.shape)

    return jax.shard_map(local_attn, mesh=mesh, in_specs=(seq_spec,) * 4, out_specs=(seq_spec,) * 4, check_vma=False)
```

```python
import functools

import jax
import jax.numpy as jnp
from jax import lax
from jax.experimental import pallas as pl
from jax.experimental.pallas import tpu as pltpu
from jax.sharding import PartitionSpec as P

OWN, Y1, AT, AO, A2, BT, BO, B2, Y2 = 0, 1, 3, 4, 7, 10, 11, 14, 16
PY1, PAT, PAO, PA2, PS, PBT, PBO, PB2 = 2, 5, 6, 8, 9, 12, 13, 15
N_SLOT = 17
ROW = 8
N_DEV = 128
CH = 256
NQ = 1024
HD = 128
TILE = 256
NEG_BIG = -1e30
LOG2E = 1.4426950408889634
SCALE = HD ** -0.5
F32 = jnp.float32
BF16 = jnp.bfloat16


def dot(a, b):
    return lax.dot_general(a, b, (((1,), (0,)), ((), ())), preferred_element_type=F32)


def kernel(q_hbm, k_hbm, v_hbm, do_hbm, o_hbm, dq_hbm, dk_hbm, dv_hbm,
           kv, q_s, do_s, qt_s, dot_s, p_buf, dp_buf, mh, m_s, l_s, d_s, ot_s, dqt_s, part,
           dr, rx, o_s, dq_s, dkv_s,
           al_s, pb_s, lsem, fs, fr, bs, br):
    me = lax.axis_index('ctx')
    core = lax.rem(me, 2)
    x = lax.rem(lax.div(me, 2), 4)
    odd = lax.rem(x, 2)
    base = me - 2 * x
    x_left = lax.rem(x + 3, 4)
    x_right = lax.rem(x + 1, 4)
    x_f = x_left + odd * (x_right - x_left)
    x_g = x_right + odd * (x_left - x_right)
    x_2 = lax.rem(x + 2, 4)
    dev_f = base + 2 * x_f
    dev_g = base + 2 * x_g
    dev_2 = base + 2 * x_2
    partner = me + 1 - 2 * core
    up = lax.rem(me + ROW, N_DEV)
    down = lax.rem(me + N_DEV - ROW, N_DEV)

    def dev(d):
        return {'dp': 0, 'ctx': d}

    loads = [
        pltpu.make_async_copy(k_hbm, kv.at[OWN, 0], lsem.at[0]),
        pltpu.make_async_copy(v_hbm, kv.at[OWN, 1], lsem.at[1]),
        pltpu.make_async_copy(q_hbm, q_s, lsem.at[2]),
        pltpu.make_async_copy(do_hbm, do_s, lsem.at[3]),
    ]
    for c in loads:
        c.start()

    row = lax.div(me, ROW)
    has_up = row < N_DEV // ROW - 1
    e1 = row >= 1
    e2 = row >= 2
    e_bt = jnp.logical_or(x_g < x, e2)
    e_bo = jnp.logical_or(x_f < x, e2)
    e_b2 = jnp.logical_or(x_2 < x, e2)

    barrier = pltpu.get_barrier_semaphore()

    def greet(d):
        pl.semaphore_signal(barrier, inc=1, device_id=dev(d), device_id_type=pl.DeviceIdType.MESH)

    pl.when(has_up)(lambda: greet(up))
    pl.when(e1)(lambda: greet(down))
    for d in (dev_f, dev_g, dev_2, partner):
        greet(d)
    pl.semaphore_wait(barrier, 4 + has_up.astype(jnp.int32) + e1.astype(jnp.int32))

    def kv_copy(msg, src, dst, d, j):
        return pltpu.make_async_remote_copy(
            src_ref=kv.at[src, j], dst_ref=kv.at[dst, j], send_sem=fs.at[msg, j], recv_sem=fr.at[dst, j],
            device_id=dev(d), device_id_type=pl.DeviceIdType.MESH)

    def kv_wait(slot, j):
        kv_copy(0, slot, slot, partner, j).wait_recv()

    def kv_send(msg, src, dst, d, j):
        kv_copy(msg, src, dst, d, j).start()

    M_Y1, M_Y2, M_AT, M_AO, M_A2, M_BT, M_BO, M_B2 = range(8)
    M_P = {PY1: 8, PAT: 9, PAO: 10, PA2: 11, PBT: 12, PBO: 13, PB2: 14, PS: 15}

    def to_partner(src, dst, j):
        kv_send(M_P[dst], src, dst, partner, j)

    for j in range(2):
        loads[j].wait()
        pl.when(has_up)(lambda: kv_send(M_Y1, OWN, Y1, up, j))
        pl.when(x_g > x)(lambda: kv_send(M_BT, OWN, BT, dev_g, j))
        pl.when(x_f > x)(lambda: kv_send(M_BO, OWN, BO, dev_f, j))
        pl.when(x_2 > x)(lambda: kv_send(M_B2, OWN, B2, dev_2, j))
        pl.when(core == 0)(lambda: to_partner(OWN, PS, j))

    loads[2].wait()
    loads[3].wait()
    for t in range(NQ // TILE):
        rows = pl.ds(t * TILE, TILE)
        qt_s[:, rows] = q_s[rows, :].T
        dot_s[:, rows] = do_s[rows, :].T
    m_s[...] = jnp.full_like(m_s, NEG_BIG)
    l_s[...] = jnp.zeros_like(l_s)
    ot_s[...] = jnp.zeros_like(ot_s)
    dqt_s[...] = jnp.zeros_like(dqt_s)

    def fwd_compute(slot, kind):
        kb = kv[slot, 0]
        vb = kv[slot, 1]
        vt = vb.T
        for t in range(NQ // TILE):
            ls = pl.ds(t * TILE, TILE)
            s = dot(kb, qt_s[:, ls])
            if kind is not None:
                key = lax.broadcasted_iota(jnp.int32, (CH, TILE), 0)
                tok = lax.shift_right_logical(lax.broadcasted_iota(jnp.int32, (CH, TILE), 1) + t * TILE, 2)
                keep = key <= tok if kind == 'own' else key > tok
                s = jnp.where(keep, s, NEG_BIG)
            p_buf[slot, :, ls] = s
            mh[slot, :, ls] = jnp.maximum(m_s[:, ls], jnp.max(s, axis=0, keepdims=True) * (SCALE * LOG2E))
        for t in range(NQ // TILE):
            ls = pl.ds(t * TILE, TILE)
            m_old = m_s[:, ls]
            m_new = mh[slot, :, ls]
            p = jnp.exp2(p_buf[slot, :, ls] * (SCALE * LOG2E) - m_new)
            p_buf[slot, :, ls] = p
            alpha = jnp.exp2(m_old - m_new)
            m_s[:, ls] = m_new
            l_s[:, ls] = l_s[:, ls] * alpha + jnp.sum(p, axis=0, keepdims=True)
            al_s[:, ls] = alpha
            dp_buf[slot, :, ls] = dot(vb, dot_s[:, ls])
            pb_s[:, ls] = p.astype(BF16)
        for t in range(NQ // TILE):
            ls = pl.ds(t * TILE, TILE)
            ot_s[:, ls] = ot_s[:, ls] * al_s[:, ls] + dot(vt, pb_s[:, ls])

    fwd_compute(OWN, 'own')

    def here(i):
        n = jnp.int32(0)
        for slots, e in (((Y1, PY1, AT, AO, PAT, PAO, A2, PA2), e1), ((BT, PBT), e_bt), ((BO, PBO), e_bo),
                         ((B2, PB2), e_b2), ((PS,), jnp.logical_or(core == 1, e2)), ((OWN,), row >= 0), ((Y2,), e2)):
            for slot in slots:
                n = n + (i == slot).astype(jnp.int32) * e.astype(jnp.int32)
        return n > 0

    def take(slot, partner_slot, e):
        @pl.when(e)
        def _():
            for j in range(2):
                kv_wait(slot, j)
                to_partner(slot, partner_slot, j)

    def fwd_body(i, carry):
        @pl.when(jnp.logical_and(i == PY1, x >= 2))
        def _():
            for j in range(2):
                kv_wait(B2, j)
                pl.when(has_up)(lambda: kv_send(M_B2, B2, A2, up, j))
                to_partner(B2, PB2, j)

        pl.when(i == PBT)(lambda: take(B2, PB2, jnp.logical_and(x < 2, e2)))

        @pl.when(here(i))
        def _():
            @pl.when(i == Y1)
            def _():
                for j in range(2):
                    kv_wait(Y1, j)
                    pl.when(has_up)(lambda: kv_send(M_Y2, Y1, Y2, up, j))
                    pl.when(x >= 2)(lambda: kv_send(M_A2, Y1, A2, dev_2, j))
                    kv_send(M_AT, Y1, AT, dev_f, j)
                    kv_send(M_AO, Y1, AO, dev_g, j)
                    to_partner(Y1, PY1, j)

            @pl.when(i == AT)
            def _():
                for j in range(2):
                    @pl.when(x < 2)
                    def _():
                        kv_wait(A2, j)
                        pl.when(has_up)(lambda: kv_send(M_A2, A2, B2, up, j))
                        to_partner(A2, PA2, j)

                    kv_wait(AT, j)
                    to_partner(AT, PAT, j)
                    kv_wait(AO, j)
                    to_partner(AO, PAO, j)

                    @pl.when(e2)
                    def _():
                        kv_wait(Y2, j)
                        pl.when(x_g < x)(lambda: kv_send(M_BT, Y2, BT, dev_g, j))
                        pl.when(x_f < x)(lambda: kv_send(M_BO, Y2, BO, dev_f, j))
                        pl.when(core == 1)(lambda: to_partner(Y2, PS, j))

            @pl.when(i == A2)
            def _():
                @pl.when(x >= 2)
                def _():
                    for j in range(2):
                        kv_wait(A2, j)
                        to_partner(A2, PA2, j)

            is_p = jnp.int32(0)
            for slot in M_P:
                is_p = is_p + (i == slot).astype(jnp.int32)

            @pl.when(is_p > 0)
            def _():
                kv_wait(i, 0)
                kv_wait(i, 1)

            fwd_compute(i, None)

        return carry

    lax.fori_loop(1, BT, fwd_body, 0)
    pl.when(e2)(lambda: fwd_compute(Y2, 'far'))
    take(BT, PBT, e_bt)
    take(BO, PBO, e_bo)
    lax.fori_loop(BT, N_SLOT - 1, fwd_body, 0)

    for t in range(NQ // TILE):
        ls = pl.ds(t * TILE, TILE)
        rl = 1.0 / l_s[:, ls]
        l_s[:, ls] = rl
        d_s[:, ls] = jnp.sum(ot_s[:, ls] * dot_s[:, ls].astype(F32), axis=0, keepdims=True) * rl

    def part_copy(msg, src, dst_ref, d, j, sem):
        return pltpu.make_async_remote_copy(
            src_ref=part.at[src, j], dst_ref=dst_ref, send_sem=bs.at[msg, j], recv_sem=br.at[sem, j],
            device_id=dev(d), device_id_type=pl.DeviceIdType.MESH)

    R_A2, R_B2, R_AT, R_AO, R_BT, R_BO, R_Y2, R_YA = range(8)

    def give(src, n):
        for j in (1, 0):
            part_copy(n, src, dr.at[n, j], partner, j, n).start()

    def got(n, j):
        part_copy(n, 0, dr.at[n, j], partner, j, n).wait_recv()

    def send(src, n, d, j):
        part_copy(8 + n, src, rx.at[n, j], d, j, 8 + n).start()

    def recv(n, j):
        part_copy(8 + n, 0, rx.at[n, j], partner, j, 8 + n).wait_recv()

    D_SLOT = {PY1: 0, PAT: 1, PAO: 2, PA2: 3, PBT: 4, PBO: 5, PB2: 6, PS: 7}

    def merge_send(slot, n_d, n_r, d):
        for j in (1, 0):
            got(n_d, j)
            part[slot, j] += dr[n_d, j]
            send(slot, n_r, d, j)

    def bwd_compute(i):
        kb = kv[i, 0]
        kt = kb.T
        dk = jnp.zeros((CH, HD), F32)
        dv = jnp.zeros((CH, HD), F32)
        for t in range(NQ // TILE):
            ls = pl.ds(t * TILE, TILE)
            f = jnp.exp2(mh[i, :, ls] - m_s[:, ls]) * l_s[:, ls]
            p = p_buf[i, :, ls] * f
            dv = dv + dot(p.astype(BF16), do_s[ls, :])
            ds = (p * (dp_buf[i, :, ls] - d_s[:, ls])).astype(BF16)
            dk = dk + dot(ds, q_s[ls, :])
            dqt_s[:, ls] += dot(kt, ds)
        part[i, 0] = dk * SCALE
        part[i, 1] = dv

        for slot, n in D_SLOT.items():
            @pl.when(i == slot)
            def _(slot=slot, n=n):
                give(slot, n)

        @pl.when(i == B2)
        def _():
            merge_send(B2, 6, R_B2, dev_g)

        @pl.when(i == BT)
        def _():
            merge_send(BT, 4, R_BT, dev_g)

        @pl.when(i == A2)
        def _():
            merge_send(A2, 3, R_A2, dev_f)

        @pl.when(i == AT)
        def _():
            merge_send(AT, 1, R_AT, dev_f)

    def bwd_body(t0, carry):
        i = lax.rem(2 * N_SLOT - 2 - t0, N_SLOT)
        pl.when(here(i))(lambda: bwd_compute(i))

        @pl.when(jnp.logical_and(i == AO, e_bo))
        def _():
            relay(BO, 5, R_B2, R_BO, dev_f)

        return carry

    def relay(slot, n_d, n_in, n_out, d):
        for j in (1, 0):
            got(n_d, j)
            recv(n_in, j)
            part[slot, j] += dr[n_d, j] + rx[n_in, j]
            send(slot, n_out, d, j)

    lax.fori_loop(0, N_SLOT, bwd_body, 0)
    pl.when(e1)(lambda: relay(AO, 2, R_A2, R_AO, dev_g))

    for t in range(NQ // TILE):
        ls = pl.ds(t * TILE, TILE)
        o_s[ls, :] = (ot_s[:, ls] * l_s[:, ls]).T.astype(BF16)
        dq_s[ls, :] = (dqt_s[:, ls] * SCALE).T.astype(BF16)
    o_out = pltpu.make_async_copy(o_s, o_hbm, lsem.at[4])
    o_out.start()
    dq_out = pltpu.make_async_copy(dq_s, dq_hbm, lsem.at[5])
    dq_out.start()

    def home_or_far(far):
        return far.astype(jnp.int32) * Y2

    def add_rx(slot, n, j):
        recv(n, j)
        part[slot, j] += rx[n, j]

    r_bt = jnp.logical_or(x < x_g, e2)
    r_bo = jnp.logical_or(x < x_f, e2)
    r_ps = jnp.logical_or(core == 0, e2)
    r_y2 = jnp.logical_and(has_up, e1)
    for j in (1, 0):
        @pl.when(r_ps)
        def _():
            got(7, j)
            part[core * Y2, j] += dr[7, j]

        pl.when(r_bt)(lambda: add_rx(home_or_far(x_g < x), R_BT, j))
        pl.when(r_bo)(lambda: add_rx(home_or_far(x_f < x), R_BO, j))
        pl.when(e2)(lambda: send(Y2, R_Y2, down, j))
    for j in (1, 0):
        @pl.when(e1)
        def _():
            got(0, j)
            part[Y1, j] += dr[0, j]
            add_rx(Y1, R_AT, j)
            add_rx(Y1, R_AO, j)
            pl.when(has_up)(lambda: add_rx(Y1, R_Y2, j))
            send(Y1, R_YA, down, j)
    outs = []
    for j, hbm in ((1, dv_hbm), (0, dk_hbm)):
        pl.when(has_up)(lambda: add_rx(OWN, R_YA, j))
        dkv_s[j] = part[OWN, j].astype(BF16)
        c = pltpu.make_async_copy(dkv_s.at[j], hbm, lsem.at[6 + j])
        c.start()
        outs.append(c)

    up1 = jnp.logical_and(has_up, e1)
    kv_sent = ((M_Y1, has_up), (M_Y2, up1), (M_AT, e1), (M_AO, e1), (M_A2, jnp.logical_and(e1, jnp.logical_or(x >= 2, has_up))),
               (M_BT, jnp.logical_or(x_g > x, e2)), (M_BO, jnp.logical_or(x_f > x, e2)), (M_B2, jnp.logical_or(x < 2, has_up)),
               (M_P[PY1], e1), (M_P[PAT], e1), (M_P[PAO], e1), (M_P[PA2], e1), (M_P[PBT], e_bt), (M_P[PBO], e_bo),
               (M_P[PB2], e_b2), (M_P[PS], r_ps))
    part_sent = ((0, e1), (1, e1), (2, e1), (3, e1), (4, e_bt), (5, e_bo), (6, e_b2), (7, jnp.logical_or(core == 1, e2)),
                 (8 + R_A2, e1), (8 + R_B2, e_b2), (8 + R_AT, e1), (8 + R_AO, e1), (8 + R_BT, e_bt), (8 + R_BO, e_bo),
                 (8 + R_Y2, e2), (8 + R_YA, e1))
    for j in range(2):
        for msg, e in kv_sent:
            pl.when(e)(lambda: kv_copy(msg, 0, 0, partner, j).wait_send())
        for msg, e in part_sent:
            pl.when(e)(lambda: part_copy(msg, 0, dr.at[0, j], partner, j, 0).wait_send())
    o_out.wait()
    dq_out.wait()
    for c in outs:
        c.wait()


def solution(mesh):
    seq_spec = P('dp', 'ctx', None, None)

    def local_attn(q_loc, k_loc, v_loc, do_loc):
        q = q_loc.reshape(NQ, HD)
        do = do_loc.reshape(NQ, HD)
        k = k_loc.reshape(CH, HD)
        v = v_loc.reshape(CH, HD)
        anyspec = pl.BlockSpec(memory_space=pl.ANY)
        o, dq, dk, dv = pl.pallas_call(
            kernel,
            out_shape=(jax.ShapeDtypeStruct((NQ, HD), BF16), jax.ShapeDtypeStruct((NQ, HD), BF16),
                       jax.ShapeDtypeStruct((CH, HD), BF16), jax.ShapeDtypeStruct((CH, HD), BF16)),
            in_specs=[anyspec] * 4,
            out_specs=[anyspec] * 4,
            scratch_shapes=[
                pltpu.VMEM((N_SLOT, 2, CH, HD), BF16),
                pltpu.VMEM((NQ, HD), BF16),
                pltpu.VMEM((NQ, HD), BF16),
                pltpu.VMEM((HD, NQ), BF16),
                pltpu.VMEM((HD, NQ), BF16),
                pltpu.VMEM((N_SLOT, CH, NQ), F32),
                pltpu.VMEM((N_SLOT, CH, NQ), F32),
                pltpu.VMEM((N_SLOT, 1, NQ), F32),
                pltpu.VMEM((1, NQ), F32),
                pltpu.VMEM((1, NQ), F32),
                pltpu.VMEM((1, NQ), F32),
                pltpu.VMEM((HD, NQ), F32),
                pltpu.VMEM((HD, NQ), F32),
                pltpu.VMEM((N_SLOT, 2, CH, HD), F32),
                pltpu.VMEM((8, 2, CH, HD), F32),
                pltpu.VMEM((8, 2, CH, HD), F32),
                pltpu.VMEM((NQ, HD), BF16),
                pltpu.VMEM((NQ, HD), BF16),
                pltpu.VMEM((2, CH, HD), BF16),
                pltpu.VMEM((1, NQ), F32),
                pltpu.VMEM((CH, NQ), BF16),
                pltpu.SemaphoreType.DMA((8,)),
                pltpu.SemaphoreType.DMA((16, 2)),
                pltpu.SemaphoreType.DMA((N_SLOT, 2)),
                pltpu.SemaphoreType.DMA((16, 2)),
                pltpu.SemaphoreType.DMA((16, 2)),
            ],
            compiler_params=pltpu.CompilerParams(
                collective_id=0, has_side_effects=True, vmem_limit_bytes=63 * 1024 * 1024),
            name='swa_fwd_bwd',
        )(q, k, v, do)
        return o.reshape(q_loc.shape), dq.reshape(q_loc.shape), dk.reshape(k_loc.shape), dv.reshape(k_loc.shape)

    return jax.shard_map(local_attn, mesh=mesh, in_specs=(seq_spec,) * 4, out_specs=(seq_spec,) * 4, check_vma=False)
```

```python
import functools

import jax
import jax.numpy as jnp
from jax import lax
from jax.experimental import pallas as pl
from jax.experimental.pallas import tpu as pltpu
from jax.sharding import PartitionSpec as P

OWN, Y1, AT, AO, A2, BT, BO, B2, Y2 = 0, 1, 3, 4, 7, 10, 11, 14, 16
PY1, PAT, PAO, PA2, PS, PBT, PBO, PB2 = 2, 5, 6, 8, 9, 12, 13, 15
N_SLOT = 17
ROW = 8
N_DEV = 128
CH = 256
NQ = 1024
HD = 128
TILE = 256
NEG_BIG = -1e30
LOG2E = 1.4426950408889634
SCALE = HD ** -0.5
F32 = jnp.float32
BF16 = jnp.bfloat16


def dot(a, b):
    return lax.dot_general(a, b, (((1,), (0,)), ((), ())), preferred_element_type=F32)


def kernel(q_hbm, k_hbm, v_hbm, do_hbm, o_hbm, dq_hbm, dk_hbm, dv_hbm,
           kv, q_s, do_s, qt_s, dot_s, p_buf, dp_buf, mh, m_s, l_s, d_s, ot_s, dqt_s, part,
           dr, rx, o_s, dq_s, dkv_s,
           al_s, pb_s, lsem, fs, fr, bs, br):
    me = lax.axis_index('ctx')
    core = lax.rem(me, 2)
    x = lax.rem(lax.div(me, 2), 4)
    odd = lax.rem(x, 2)
    base = me - 2 * x
    x_left = lax.rem(x + 3, 4)
    x_right = lax.rem(x + 1, 4)
    x_f = x_left + odd * (x_right - x_left)
    x_g = x_right + odd * (x_left - x_right)
    x_2 = lax.rem(x + 2, 4)
    dev_f = base + 2 * x_f
    dev_g = base + 2 * x_g
    dev_2 = base + 2 * x_2
    partner = me + 1 - 2 * core
    up = lax.rem(me + ROW, N_DEV)
    down = lax.rem(me + N_DEV - ROW, N_DEV)

    def dev(d):
        return {'dp': 0, 'ctx': d}

    loads = [
        pltpu.make_async_copy(k_hbm, kv.at[OWN, 0], lsem.at[0]),
        pltpu.make_async_copy(v_hbm, kv.at[OWN, 1], lsem.at[1]),
        pltpu.make_async_copy(q_hbm, q_s, lsem.at[2]),
        pltpu.make_async_copy(do_hbm, do_s, lsem.at[3]),
    ]
    for c in loads:
        c.start()

    row = lax.div(me, ROW)
    has_up = row < N_DEV // ROW - 1
    e1 = row >= 1
    e2 = row >= 2
    e_bt = jnp.logical_or(x_g < x, e2)
    e_bo = jnp.logical_or(x_f < x, e2)
    e_b2 = jnp.logical_or(x_2 < x, e2)

    barrier = pltpu.get_barrier_semaphore()

    def greet(d):
        pl.semaphore_signal(barrier, inc=1, device_id=dev(d), device_id_type=pl.DeviceIdType.MESH)

    pl.when(has_up)(lambda: greet(up))
    pl.when(e1)(lambda: greet(down))
    for d in (dev_f, dev_g, dev_2, partner):
        greet(d)
    pl.semaphore_wait(barrier, 4 + has_up.astype(jnp.int32) + e1.astype(jnp.int32))

    def kv_copy(msg, src, dst, d, j):
        return pltpu.make_async_remote_copy(
            src_ref=kv.at[src, j], dst_ref=kv.at[dst, j], send_sem=fs.at[msg, j], recv_sem=fr.at[dst, j],
            device_id=dev(d), device_id_type=pl.DeviceIdType.MESH)

    def kv_wait(slot, j):
        kv_copy(0, slot, slot, partner, j).wait_recv()

    def kv_send(msg, src, dst, d, j):
        kv_copy(msg, src, dst, d, j).start()

    M_Y1, M_Y2, M_AT, M_AO, M_A2, M_BT, M_BO, M_B2 = range(8)
    M_P = {PY1: 8, PAT: 9, PAO: 10, PA2: 11, PBT: 12, PBO: 13, PB2: 14, PS: 15}

    def to_partner(src, dst, j):
        kv_send(M_P[dst], src, dst, partner, j)

    for j in range(2):
        loads[j].wait()
        pl.when(has_up)(lambda: kv_send(M_Y1, OWN, Y1, up, j))
        pl.when(x_g > x)(lambda: kv_send(M_BT, OWN, BT, dev_g, j))
        pl.when(x_f > x)(lambda: kv_send(M_BO, OWN, BO, dev_f, j))
        pl.when(x_2 > x)(lambda: kv_send(M_B2, OWN, B2, dev_2, j))
        pl.when(core == 0)(lambda: to_partner(OWN, PS, j))

    loads[2].wait()
    loads[3].wait()
    for t in range(NQ // TILE):
        rows = pl.ds(t * TILE, TILE)
        qt_s[:, rows] = q_s[rows, :].T
        dot_s[:, rows] = do_s[rows, :].T
    m_s[...] = jnp.full_like(m_s, NEG_BIG)
    l_s[...] = jnp.zeros_like(l_s)
    ot_s[...] = jnp.zeros_like(ot_s)
    dqt_s[...] = jnp.zeros_like(dqt_s)

    def fwd_compute(slot, kind):
        kb = kv[slot, 0]
        vb = kv[slot, 1]
        vt = vb.T
        for t in range(NQ // TILE):
            ls = pl.ds(t * TILE, TILE)
            s = dot(kb, qt_s[:, ls])
            if kind is not None:
                key = lax.broadcasted_iota(jnp.int32, (CH, TILE), 0)
                tok = lax.shift_right_logical(lax.broadcasted_iota(jnp.int32, (CH, TILE), 1) + t * TILE, 2)
                keep = key <= tok if kind == 'own' else key > tok
                s = jnp.where(keep, s, NEG_BIG)
            p_buf[slot, :, ls] = s
            mh[slot, :, ls] = jnp.maximum(m_s[:, ls], jnp.max(s, axis=0, keepdims=True) * (SCALE * LOG2E))
        for t in range(NQ // TILE):
            ls = pl.ds(t * TILE, TILE)
            m_old = m_s[:, ls]
            m_new = mh[slot, :, ls]
            p = jnp.exp2(p_buf[slot, :, ls] * (SCALE * LOG2E) - m_new)
            p_buf[slot, :, ls] = p
            alpha = jnp.exp2(m_old - m_new)
            m_s[:, ls] = m_new
            l_s[:, ls] = l_s[:, ls] * alpha + jnp.sum(p, axis=0, keepdims=True)
            al_s[:, ls] = alpha
            dp_buf[slot, :, ls] = dot(vb, dot_s[:, ls])
            pb_s[:, ls] = p.astype(BF16)
        for t in range(NQ // TILE):
            ls = pl.ds(t * TILE, TILE)
            ot_s[:, ls] = ot_s[:, ls] * al_s[:, ls] + dot(vt, pb_s[:, ls])

    fwd_compute(OWN, 'own')

    def here(i):
        n = jnp.int32(0)
        for slots, e in (((Y1, PY1, AT, AO, PAT, PAO, A2, PA2), e1), ((BT, PBT), e_bt), ((BO, PBO), e_bo),
                         ((B2, PB2), e_b2), ((PS,), jnp.logical_or(core == 1, e2)), ((OWN,), row >= 0), ((Y2,), e2)):
            for slot in slots:
                n = n + (i == slot).astype(jnp.int32) * e.astype(jnp.int32)
        return n > 0

    def take(slot, partner_slot, e):
        @pl.when(e)
        def _():
            for j in range(2):
                kv_wait(slot, j)
                to_partner(slot, partner_slot, j)

    def fwd_body(i, carry):
        @pl.when(jnp.logical_and(i == PY1, x >= 2))
        def _():
            for j in range(2):
                kv_wait(B2, j)
                pl.when(has_up)(lambda: kv_send(M_B2, B2, A2, up, j))
                to_partner(B2, PB2, j)

        pl.when(i == PBT)(lambda: take(B2, PB2, jnp.logical_and(x < 2, e2)))

        @pl.when(here(i))
        def _():
            @pl.when(i == Y1)
            def _():
                for j in range(2):
                    kv_wait(Y1, j)
                    pl.when(has_up)(lambda: kv_send(M_Y2, Y1, Y2, up, j))
                    pl.when(x >= 2)(lambda: kv_send(M_A2, Y1, A2, dev_2, j))
                    kv_send(M_AT, Y1, AT, dev_f, j)
                    kv_send(M_AO, Y1, AO, dev_g, j)
                    to_partner(Y1, PY1, j)

            @pl.when(i == AT)
            def _():
                for j in range(2):
                    @pl.when(x < 2)
                    def _():
                        kv_wait(A2, j)
                        pl.when(has_up)(lambda: kv_send(M_A2, A2, B2, up, j))
                        to_partner(A2, PA2, j)

                    kv_wait(AT, j)
                    to_partner(AT, PAT, j)
                    kv_wait(AO, j)
                    to_partner(AO, PAO, j)

                    @pl.when(e2)
                    def _():
                        kv_wait(Y2, j)
                        pl.when(x_g < x)(lambda: kv_send(M_BT, Y2, BT, dev_g, j))
                        pl.when(x_f < x)(lambda: kv_send(M_BO, Y2, BO, dev_f, j))
                        pl.when(core == 1)(lambda: to_partner(Y2, PS, j))

            @pl.when(i == A2)
            def _():
                @pl.when(x >= 2)
                def _():
                    for j in range(2):
                        kv_wait(A2, j)
                        to_partner(A2, PA2, j)

            is_p = jnp.int32(0)
            for slot in M_P:
                is_p = is_p + (i == slot).astype(jnp.int32)

            @pl.when(is_p > 0)
            def _():
                kv_wait(i, 0)
                kv_wait(i, 1)

            fwd_compute(i, None)

        return carry

    lax.fori_loop(1, BT, fwd_body, 0)
    pl.when(e2)(lambda: fwd_compute(Y2, 'far'))
    take(BT, PBT, e_bt)
    take(BO, PBO, e_bo)
    lax.fori_loop(BT, N_SLOT - 1, fwd_body, 0)

    for t in range(NQ // TILE):
        ls = pl.ds(t * TILE, TILE)
        rl = 1.0 / l_s[:, ls]
        l_s[:, ls] = rl
        d_s[:, ls] = jnp.sum(ot_s[:, ls] * dot_s[:, ls].astype(F32), axis=0, keepdims=True) * rl

    def part_copy(msg, src, dst_ref, d, q, sem):
        return pltpu.make_async_remote_copy(
            src_ref=part.at[src, q], dst_ref=dst_ref, send_sem=bs.at[msg, q], recv_sem=br.at[sem, q],
            device_id=dev(d), device_id_type=pl.DeviceIdType.MESH)

    R_DN, R_2, R_AT, R_AO, R_BT, R_BO, R_Y2, R_YA = range(8)
    ORDER = (2, 3, 0, 1)

    def give(src, n):
        for q in ORDER:
            part_copy(n, src, dr.at[n, q], partner, q, n).start()

    def add_dr(slot, n, q):
        part_copy(n, 0, dr.at[n, q], partner, q, n).wait_recv()
        part[slot, q] += dr[n, q]

    def send(src, n, d, q):
        part_copy(8 + n, src, rx.at[n, q], d, q, 8 + n).start()

    def add_rx(slot, n, q):
        part_copy(8 + n, 0, rx.at[n, q], partner, q, 8 + n).wait_recv()
        part[slot, q] += rx[n, q]

    D_SLOT = {PY1: 0, PAT: 1, PAO: 2, PA2: 3, PBT: 4, PBO: 5, PB2: 6, PS: 7}

    def merge_send(slot, n_d, n_r, d):
        for q in ORDER:
            add_dr(slot, n_d, q)
            send(slot, n_r, d, q)

    hi = (x >= 2).astype(jnp.int32)
    low = x < 2
    s_dn, n_dn = B2 + hi * (A2 - B2), 6 - hi * 3
    s_x2, n_x2 = A2 + hi * (B2 - A2), 3 + hi * 3
    e_dn = jnp.logical_or(jnp.logical_and(low, e2), jnp.logical_and(x >= 2, e1))
    e_x2 = jnp.logical_or(x >= 2, e1)
    r_dn = jnp.logical_and(has_up, e_x2)
    r_x2 = jnp.logical_or(low, e1)

    B_ORDER = (PBT, PBO, BT, BO, PB2, PA2, B2, A2, PAT, PAO, AT, AO, PS, Y2, PY1, Y1, OWN)

    def bwd_compute(i):
        kb = kv[i, 0]
        kt = kb.T
        dk = jnp.zeros((CH, HD), F32)
        dv = jnp.zeros((CH, HD), F32)
        for t in range(NQ // TILE):
            ls = pl.ds(t * TILE, TILE)
            f = jnp.exp2(mh[i, :, ls] - m_s[:, ls]) * l_s[:, ls]
            p = p_buf[i, :, ls] * f
            dv = dv + dot(p.astype(BF16), do_s[ls, :])
            ds = (p * (dp_buf[i, :, ls] - d_s[:, ls])).astype(BF16)
            dk = dk + dot(ds, q_s[ls, :])
            dqt_s[:, ls] += dot(kt, ds)
        half = CH // 2
        part[i, 0] = dk[:half] * SCALE
        part[i, 1] = dk[half:] * SCALE
        part[i, 2] = dv[:half]
        part[i, 3] = dv[half:]

        for slot, n in D_SLOT.items():
            @pl.when(i == slot)
            def _(slot=slot, n=n):
                give(slot, n)

        @pl.when(i == AT)
        def _():
            merge_send(AT, 1, R_AT, dev_f)

        @pl.when(i == AO)
        def _():
            merge_send(AO, 2, R_AO, dev_g)

        @pl.when(i == Y1)
        def _():
            for q in ORDER:
                add_dr(Y1, 0, q)

    def bwd_body(t0, carry):
        i = jnp.int32(0)
        for t, slot in enumerate(B_ORDER):
            i = i + (t0 == t).astype(jnp.int32) * slot
        pl.when(here(i))(lambda: bwd_compute(i))

        @pl.when(i == PB2)
        def _():
            pl.when(e_bt)(lambda: merge_send(BT, 4, R_BT, dev_g))
            pl.when(e_bo)(lambda: merge_send(BO, 5, R_BO, dev_f))

        @pl.when(jnp.logical_and(i == PAO, e_dn))
        def _():
            merge_send(s_dn, n_dn, R_DN, down)

        return carry

    lax.fori_loop(0, N_SLOT, bwd_body, 0)

    def home_or_far(far):
        return far.astype(jnp.int32) * Y2

    r_bt = jnp.logical_or(x < x_g, e2)
    r_bo = jnp.logical_or(x < x_f, e2)
    r_ps = jnp.logical_or(core == 0, e2)
    r_y2 = jnp.logical_and(has_up, e1)

    for q in ORDER:
        @pl.when(e_x2)
        def _():
            add_dr(s_x2, n_x2, q)
            pl.when(r_dn)(lambda: add_rx(s_x2, R_DN, q))
            send(s_x2, R_2, dev_2, q)

    for q in ORDER:
        pl.when(r_ps)(lambda: add_dr(core * Y2, 7, q))
        pl.when(r_bt)(lambda: add_rx(home_or_far(x_g < x), R_BT, q))
        pl.when(r_bo)(lambda: add_rx(home_or_far(x_f < x), R_BO, q))
        pl.when(e2)(lambda: send(Y2, R_Y2, down, q))

    for t in range(NQ // TILE):
        ls = pl.ds(t * TILE, TILE)
        o_s[ls, :] = (ot_s[:, ls] * l_s[:, ls]).T.astype(BF16)
        dq_s[ls, :] = (dqt_s[:, ls] * SCALE).T.astype(BF16)
    o_out = pltpu.make_async_copy(o_s, o_hbm, lsem.at[4])
    o_out.start()
    dq_out = pltpu.make_async_copy(dq_s, dq_hbm, lsem.at[5])
    dq_out.start()

    for q in ORDER:
        @pl.when(e1)
        def _():
            add_rx(Y1, R_AT, q)
            add_rx(Y1, R_AO, q)
            pl.when(has_up)(lambda: add_rx(Y1, R_Y2, q))

    for q in ORDER:
        pl.when(r_x2)(lambda: add_rx(hi * Y1, R_2, q))
        pl.when(e1)(lambda: send(Y1, R_YA, down, q))
    for q in ORDER:
        pl.when(has_up)(lambda: add_rx(OWN, R_YA, q))
        dkv_s[q // 2, pl.ds(q % 2 * (CH // 2), CH // 2), :] = part[OWN, q].astype(BF16)
    outs = []
    for j, hbm in ((1, dv_hbm), (0, dk_hbm)):
        c = pltpu.make_async_copy(dkv_s.at[j], hbm, lsem.at[6 + j])
        c.start()
        outs.append(c)

    up1 = jnp.logical_and(has_up, e1)
    kv_sent = ((M_Y1, has_up), (M_Y2, up1), (M_AT, e1), (M_AO, e1), (M_A2, jnp.logical_and(e1, jnp.logical_or(x >= 2, has_up))),
               (M_BT, jnp.logical_or(x_g > x, e2)), (M_BO, jnp.logical_or(x_f > x, e2)), (M_B2, jnp.logical_or(x < 2, has_up)),
               (M_P[PY1], e1), (M_P[PAT], e1), (M_P[PAO], e1), (M_P[PA2], e1), (M_P[PBT], e_bt), (M_P[PBO], e_bo),
               (M_P[PB2], e_b2), (M_P[PS], r_ps))
    part_sent = ((0, e1), (1, e1), (2, e1), (3, e1), (4, e_bt), (5, e_bo), (6, e_b2), (7, jnp.logical_or(core == 1, e2)),
                 (8 + R_DN, e_dn), (8 + R_2, e_x2), (8 + R_AT, e1), (8 + R_AO, e1), (8 + R_BT, e_bt), (8 + R_BO, e_bo),
                 (8 + R_Y2, e2), (8 + R_YA, e1))
    for j in range(2):
        for msg, e in kv_sent:
            pl.when(e)(lambda: kv_copy(msg, 0, 0, partner, j).wait_send())
    for q in range(4):
        for msg, e in part_sent:
            pl.when(e)(lambda: part_copy(msg, 0, dr.at[0, q], partner, q, 0).wait_send())
    o_out.wait()
    dq_out.wait()
    for c in outs:
        c.wait()


def solution(mesh):
    seq_spec = P('dp', 'ctx', None, None)

    def local_attn(q_loc, k_loc, v_loc, do_loc):
        q = q_loc.reshape(NQ, HD)
        do = do_loc.reshape(NQ, HD)
        k = k_loc.reshape(CH, HD)
        v = v_loc.reshape(CH, HD)
        anyspec = pl.BlockSpec(memory_space=pl.ANY)
        o, dq, dk, dv = pl.pallas_call(
            kernel,
            out_shape=(jax.ShapeDtypeStruct((NQ, HD), BF16), jax.ShapeDtypeStruct((NQ, HD), BF16),
                       jax.ShapeDtypeStruct((CH, HD), BF16), jax.ShapeDtypeStruct((CH, HD), BF16)),
            in_specs=[anyspec] * 4,
            out_specs=[anyspec] * 4,
            scratch_shapes=[
                pltpu.VMEM((N_SLOT, 2, CH, HD), BF16),
                pltpu.VMEM((NQ, HD), BF16),
                pltpu.VMEM((NQ, HD), BF16),
                pltpu.VMEM((HD, NQ), BF16),
                pltpu.VMEM((HD, NQ), BF16),
                pltpu.VMEM((N_SLOT, CH, NQ), F32),
                pltpu.VMEM((N_SLOT, CH, NQ), F32),
                pltpu.VMEM((N_SLOT, 1, NQ), F32),
                pltpu.VMEM((1, NQ), F32),
                pltpu.VMEM((1, NQ), F32),
                pltpu.VMEM((1, NQ), F32),
                pltpu.VMEM((HD, NQ), F32),
                pltpu.VMEM((HD, NQ), F32),
                pltpu.VMEM((N_SLOT, 4, CH // 2, HD), F32),
                pltpu.VMEM((8, 4, CH // 2, HD), F32),
                pltpu.VMEM((8, 4, CH // 2, HD), F32),
                pltpu.VMEM((NQ, HD), BF16),
                pltpu.VMEM((NQ, HD), BF16),
                pltpu.VMEM((2, CH, HD), BF16),
                pltpu.VMEM((1, NQ), F32),
                pltpu.VMEM((CH, NQ), BF16),
                pltpu.SemaphoreType.DMA((8,)),
                pltpu.SemaphoreType.DMA((16, 2)),
                pltpu.SemaphoreType.DMA((N_SLOT, 2)),
                pltpu.SemaphoreType.DMA((16, 4)),
                pltpu.SemaphoreType.DMA((16, 4)),
            ],
            compiler_params=pltpu.CompilerParams(
                collective_id=0, has_side_effects=True, vmem_limit_bytes=63 * 1024 * 1024),
            name='swa_fwd_bwd',
        )(q, k, v, do)
        return o.reshape(q_loc.shape), dq.reshape(q_loc.shape), dk.reshape(k_loc.shape), dv.reshape(k_loc.shape)

    return jax.shard_map(local_attn, mesh=mesh, in_specs=(seq_spec,) * 4, out_specs=(seq_spec,) * 4, check_vma=False)
```

```python
import functools

import jax
import jax.numpy as jnp
from jax import lax
from jax.experimental import pallas as pl
from jax.experimental.pallas import tpu as pltpu
from jax.sharding import PartitionSpec as P

OWN, Y1, AT, AO, A2, BT, BO, B2, Y2 = 0, 1, 3, 4, 7, 10, 11, 14, 16
PY1, PAT, PAO, PA2, PS, PBT, PBO, PB2 = 2, 5, 6, 8, 9, 12, 13, 15
N_SLOT = 17
ROW = 8
N_DEV = 128
CH = 256
NQ = 1024
HD = 128
TILE = 256
NEG_BIG = -1e30
LOG2E = 1.4426950408889634
SCALE = HD ** -0.5
F32 = jnp.float32
BF16 = jnp.bfloat16


def dot(a, b):
    return lax.dot_general(a, b, (((1,), (0,)), ((), ())), preferred_element_type=F32)


def kernel(q_hbm, k_hbm, v_hbm, do_hbm, o_hbm, dq_hbm, dk_hbm, dv_hbm,
           kv, q_s, do_s, qt_s, dot_s, p_buf, dp_buf, mh, m_s, l_s, d_s, ot_s, dqt_s, part,
           dr, rx, o_s, dq_s, dkv_s,
           al_s, pb_s, lsem, fs, fr, bs, br):
    me = lax.axis_index('ctx')
    core = lax.rem(me, 2)
    x = lax.rem(lax.div(me, 2), 4)
    odd = lax.rem(x, 2)
    base = me - 2 * x
    x_left = lax.rem(x + 3, 4)
    x_right = lax.rem(x + 1, 4)
    x_f = x_left + odd * (x_right - x_left)
    x_g = x_right + odd * (x_left - x_right)
    x_2 = lax.rem(x + 2, 4)
    dev_f = base + 2 * x_f
    dev_g = base + 2 * x_g
    dev_2 = base + 2 * x_2
    partner = me + 1 - 2 * core
    up = lax.rem(me + ROW, N_DEV)
    down = lax.rem(me + N_DEV - ROW, N_DEV)

    def dev(d):
        return {'dp': 0, 'ctx': d}

    loads = [
        pltpu.make_async_copy(k_hbm, kv.at[OWN, 0], lsem.at[0]),
        pltpu.make_async_copy(v_hbm, kv.at[OWN, 1], lsem.at[1]),
        pltpu.make_async_copy(q_hbm, q_s, lsem.at[2]),
        pltpu.make_async_copy(do_hbm, do_s, lsem.at[3]),
    ]
    for c in loads:
        c.start()

    row = lax.div(me, ROW)
    has_up = row < N_DEV // ROW - 1
    e1 = row >= 1
    e2 = row >= 2
    e_bt = jnp.logical_or(x_g < x, e2)
    e_bo = jnp.logical_or(x_f < x, e2)
    e_b2 = jnp.logical_or(x_2 < x, e2)

    barrier = pltpu.get_barrier_semaphore()

    def greet(d):
        pl.semaphore_signal(barrier, inc=1, device_id=dev(d), device_id_type=pl.DeviceIdType.MESH)

    pl.when(has_up)(lambda: greet(up))
    pl.when(e1)(lambda: greet(down))
    for d in (dev_f, dev_g, dev_2, partner):
        greet(d)
    pl.semaphore_wait(barrier, 4 + has_up.astype(jnp.int32) + e1.astype(jnp.int32))

    def kv_copy(msg, src, dst, d, j):
        return pltpu.make_async_remote_copy(
            src_ref=kv.at[src, j], dst_ref=kv.at[dst, j], send_sem=fs.at[msg, j], recv_sem=fr.at[dst, j],
            device_id=dev(d), device_id_type=pl.DeviceIdType.MESH)

    def kv_wait(slot, j):
        kv_copy(0, slot, slot, partner, j).wait_recv()

    def kv_send(msg, src, dst, d, j):
        kv_copy(msg, src, dst, d, j).start()

    M_Y1, M_Y2, M_AT, M_AO, M_A2, M_BT, M_BO, M_B2 = range(8)
    M_P = {PY1: 8, PAT: 9, PAO: 10, PA2: 11, PBT: 12, PBO: 13, PB2: 14, PS: 15}

    def to_partner(src, dst, j):
        kv_send(M_P[dst], src, dst, partner, j)

    for j in range(2):
        loads[j].wait()
        pl.when(has_up)(lambda: kv_send(M_Y1, OWN, Y1, up, j))
        pl.when(x_g > x)(lambda: kv_send(M_BT, OWN, BT, dev_g, j))
        pl.when(x_f > x)(lambda: kv_send(M_BO, OWN, BO, dev_f, j))
        pl.when(x_2 > x)(lambda: kv_send(M_B2, OWN, B2, dev_2, j))
        pl.when(core == 0)(lambda: to_partner(OWN, PS, j))

    loads[2].wait()
    loads[3].wait()
    for t in range(NQ // TILE):
        rows = pl.ds(t * TILE, TILE)
        qt_s[:, rows] = q_s[rows, :].T
        dot_s[:, rows] = do_s[rows, :].T
    m_s[...] = jnp.full_like(m_s, NEG_BIG)
    l_s[...] = jnp.zeros_like(l_s)
    ot_s[...] = jnp.zeros_like(ot_s)
    dqt_s[...] = jnp.zeros_like(dqt_s)

    def fwd_compute(slot, kind):
        kb = kv[slot, 0]
        vb = kv[slot, 1]
        vt = vb.T
        for t in range(NQ // TILE):
            ls = pl.ds(t * TILE, TILE)
            s = dot(kb, qt_s[:, ls])
            if kind is not None:
                key = lax.broadcasted_iota(jnp.int32, (CH, TILE), 0)
                tok = lax.shift_right_logical(lax.broadcasted_iota(jnp.int32, (CH, TILE), 1) + t * TILE, 2)
                keep = key <= tok if kind == 'own' else key > tok
                s = jnp.where(keep, s, NEG_BIG)
            p_buf[slot, :, ls] = s
            mh[slot, :, ls] = jnp.maximum(m_s[:, ls], jnp.max(s, axis=0, keepdims=True) * (SCALE * LOG2E))
        for t in range(NQ // TILE):
            ls = pl.ds(t * TILE, TILE)
            m_old = m_s[:, ls]
            m_new = mh[slot, :, ls]
            p = jnp.exp2(p_buf[slot, :, ls] * (SCALE * LOG2E) - m_new)
            p_buf[slot, :, ls] = p
            alpha = jnp.exp2(m_old - m_new)
            m_s[:, ls] = m_new
            l_s[:, ls] = l_s[:, ls] * alpha + jnp.sum(p, axis=0, keepdims=True)
            al_s[:, ls] = alpha
            dp_buf[slot, :, ls] = dot(vb, dot_s[:, ls])
            pb_s[:, ls] = p.astype(BF16)
        for t in range(NQ // TILE):
            ls = pl.ds(t * TILE, TILE)
            ot_s[:, ls] = ot_s[:, ls] * al_s[:, ls] + dot(vt, pb_s[:, ls])

    fwd_compute(OWN, 'own')

    def here(i):
        n = jnp.int32(0)
        for slots, e in (((Y1, PY1, AT, AO, PAT, PAO, A2, PA2), e1), ((BT, PBT), e_bt), ((BO, PBO), e_bo),
                         ((B2, PB2), e_b2), ((PS,), jnp.logical_or(core == 1, e2)), ((OWN,), row >= 0), ((Y2,), e2)):
            for slot in slots:
                n = n + (i == slot).astype(jnp.int32) * e.astype(jnp.int32)
        return n > 0

    def take(slot, partner_slot, e):
        @pl.when(e)
        def _():
            for j in range(2):
                kv_wait(slot, j)
                to_partner(slot, partner_slot, j)

    def fwd_body(i, carry):
        @pl.when(jnp.logical_and(i == PY1, x >= 2))
        def _():
            for j in range(2):
                kv_wait(B2, j)
                pl.when(has_up)(lambda: kv_send(M_B2, B2, A2, up, j))
                to_partner(B2, PB2, j)

        pl.when(i == PBT)(lambda: take(B2, PB2, jnp.logical_and(x < 2, e2)))

        @pl.when(here(i))
        def _():
            @pl.when(i == Y1)
            def _():
                for j in range(2):
                    kv_wait(Y1, j)
                    pl.when(has_up)(lambda: kv_send(M_Y2, Y1, Y2, up, j))
                    pl.when(x >= 2)(lambda: kv_send(M_A2, Y1, A2, dev_2, j))
                    kv_send(M_AT, Y1, AT, dev_f, j)
                    kv_send(M_AO, Y1, AO, dev_g, j)
                    to_partner(Y1, PY1, j)

            @pl.when(i == AT)
            def _():
                for j in range(2):
                    @pl.when(x < 2)
                    def _():
                        kv_wait(A2, j)
                        pl.when(has_up)(lambda: kv_send(M_A2, A2, B2, up, j))
                        to_partner(A2, PA2, j)

                    kv_wait(AT, j)
                    to_partner(AT, PAT, j)
                    kv_wait(AO, j)
                    to_partner(AO, PAO, j)

                    @pl.when(e2)
                    def _():
                        kv_wait(Y2, j)
                        pl.when(x_g < x)(lambda: kv_send(M_BT, Y2, BT, dev_g, j))
                        pl.when(x_f < x)(lambda: kv_send(M_BO, Y2, BO, dev_f, j))
                        pl.when(core == 1)(lambda: to_partner(Y2, PS, j))

            @pl.when(i == A2)
            def _():
                @pl.when(x >= 2)
                def _():
                    for j in range(2):
                        kv_wait(A2, j)
                        to_partner(A2, PA2, j)

            is_p = jnp.int32(0)
            for slot in M_P:
                is_p = is_p + (i == slot).astype(jnp.int32)

            @pl.when(is_p > 0)
            def _():
                kv_wait(i, 0)
                kv_wait(i, 1)

            fwd_compute(i, None)

        return carry

    lax.fori_loop(1, BT, fwd_body, 0)
    pl.when(e2)(lambda: fwd_compute(Y2, 'far'))
    take(BT, PBT, e_bt)
    take(BO, PBO, e_bo)
    lax.fori_loop(BT, N_SLOT - 1, fwd_body, 0)

    for t in range(NQ // TILE):
        ls = pl.ds(t * TILE, TILE)
        rl = 1.0 / l_s[:, ls]
        l_s[:, ls] = rl
        d_s[:, ls] = jnp.sum(ot_s[:, ls] * dot_s[:, ls].astype(F32), axis=0, keepdims=True) * rl

    def part_copy(msg, src, dst_ref, d, q, sem):
        return pltpu.make_async_remote_copy(
            src_ref=part.at[src, q], dst_ref=dst_ref, send_sem=bs.at[msg, q], recv_sem=br.at[sem, q],
            device_id=dev(d), device_id_type=pl.DeviceIdType.MESH)

    R_DN, R_2, R_AT, R_AO, R_BT, R_BO, R_Y2, R_YA = range(8)
    ORDER = (2, 3, 0, 1)

    def give(src, n):
        for q in ORDER:
            part_copy(n, src, dr.at[n, q], partner, q, n).start()

    def add_dr(slot, n, q):
        part_copy(n, 0, dr.at[n, q], partner, q, n).wait_recv()
        part[slot, q] += dr[n, q]

    def send(src, n, d, q):
        part_copy(8 + n, src, rx.at[n, q], d, q, 8 + n).start()

    def add_rx(slot, n, q):
        part_copy(8 + n, 0, rx.at[n, q], partner, q, 8 + n).wait_recv()
        part[slot, q] += rx[n, q]

    D_SLOT = {PY1: 0, PAT: 1, PAO: 2, PA2: 3, PBT: 4, PBO: 5, PB2: 6, PS: 7}

    def merge_send(slot, n_d, n_r, d):
        for q in ORDER:
            add_dr(slot, n_d, q)
            send(slot, n_r, d, q)

    hi = (x >= 2).astype(jnp.int32)
    low = x < 2
    s_dn, n_dn = B2 + hi * (A2 - B2), 6 - hi * 3
    s_x2, n_x2 = A2 + hi * (B2 - A2), 3 + hi * 3
    e_dn = jnp.logical_or(jnp.logical_and(low, e2), jnp.logical_and(x >= 2, e1))
    e_x2 = jnp.logical_or(x >= 2, e1)
    r_dn = jnp.logical_and(has_up, e_x2)

    B_ORDER = (PBT, PBO, PB2, PA2, BT, BO, B2, A2, PAT, PAO, PS, Y2, AT, AO, PY1, Y1, OWN)

    def bwd_compute(i):
        kb = kv[i, 0]
        kt = kb.T
        dk = jnp.zeros((CH, HD), F32)
        dv = jnp.zeros((CH, HD), F32)
        for t in range(NQ // TILE):
            ls = pl.ds(t * TILE, TILE)
            f = jnp.exp2(mh[i, :, ls] - m_s[:, ls]) * l_s[:, ls]
            p = p_buf[i, :, ls] * f
            dv = dv + dot(p.astype(BF16), do_s[ls, :])
            ds = (p * (dp_buf[i, :, ls] - d_s[:, ls])).astype(BF16)
            dk = dk + dot(ds, q_s[ls, :])
            dqt_s[:, ls] += dot(kt, ds)
        half = CH // 2
        part[i, 0] = dk[:half] * SCALE
        part[i, 1] = dk[half:] * SCALE
        part[i, 2] = dv[:half]
        part[i, 3] = dv[half:]

        for slot, n in D_SLOT.items():
            @pl.when(i == slot)
            def _(slot=slot, n=n):
                give(slot, n)

        @pl.when(i == BT)
        def _():
            merge_send(BT, 4, R_BT, dev_g)

        @pl.when(i == BO)
        def _():
            merge_send(BO, 5, R_BO, dev_f)

        @pl.when(i == AT)
        def _():
            merge_send(AT, 1, R_AT, dev_f)

        @pl.when(i == AO)
        def _():
            merge_send(AO, 2, R_AO, dev_g)

    def bwd_body(t0, carry):
        i = jnp.int32(0)
        for t, slot in enumerate(B_ORDER):
            i = i + (t0 == t).astype(jnp.int32) * slot
        pl.when(here(i))(lambda: bwd_compute(i))

        @pl.when(jnp.logical_and(i == A2, e_dn))
        def _():
            merge_send(s_dn, n_dn, R_DN, down)

        return carry

    lax.fori_loop(0, N_SLOT, bwd_body, 0)

    def home_or_far(far):
        return far.astype(jnp.int32) * Y2

    r_bt = jnp.logical_or(x < x_g, e2)
    r_bo = jnp.logical_or(x < x_f, e2)
    r_ps = jnp.logical_or(core == 0, e2)

    def cross(q, e):
        @pl.when(e)
        def _():
            add_dr(s_x2, n_x2, q)
            pl.when(r_dn)(lambda: add_rx(s_x2, R_DN, q))
            send(s_x2, R_2, dev_2, q)

    def far(q):
        pl.when(r_ps)(lambda: add_dr(core * Y2, 7, q))
        pl.when(r_bt)(lambda: add_rx(home_or_far(x_g < x), R_BT, q))
        pl.when(r_bo)(lambda: add_rx(home_or_far(x_f < x), R_BO, q))
        pl.when(e2)(lambda: send(Y2, R_Y2, down, q))

    for t in range(NQ // TILE):
        ls = pl.ds(t * TILE, TILE)
        o_s[ls, :] = (ot_s[:, ls] * l_s[:, ls]).T.astype(BF16)
        dq_s[ls, :] = (dqt_s[:, ls] * SCALE).T.astype(BF16)
    o_out = pltpu.make_async_copy(o_s, o_hbm, lsem.at[4])
    o_out.start()
    dq_out = pltpu.make_async_copy(dq_s, dq_hbm, lsem.at[5])
    dq_out.start()

    for pair in ((2, 3), (0, 1)):
        for q in pair:
            far(q)
        for q in pair:
            cross(q, jnp.logical_and(low, e1))
    for q in ORDER:
        cross(q, x >= 2)
    for q in ORDER:
        @pl.when(e1)
        def _():
            add_dr(Y1, 0, q)
            add_rx(Y1, R_AT, q)
            add_rx(Y1, R_AO, q)
            pl.when(has_up)(lambda: add_rx(Y1, R_Y2, q))
            pl.when(x >= 2)(lambda: add_rx(Y1, R_2, q))
            send(Y1, R_YA, down, q)
    for q in ORDER:
        pl.when(low)(lambda: add_rx(OWN, R_2, q))
        pl.when(has_up)(lambda: add_rx(OWN, R_YA, q))
        dkv_s[q // 2, pl.ds(q % 2 * (CH // 2), CH // 2), :] = part[OWN, q].astype(BF16)
    outs = []
    for j, hbm in ((1, dv_hbm), (0, dk_hbm)):
        c = pltpu.make_async_copy(dkv_s.at[j], hbm, lsem.at[6 + j])
        c.start()
        outs.append(c)

    up1 = jnp.logical_and(has_up, e1)
    kv_sent = ((M_Y1, has_up), (M_Y2, up1), (M_AT, e1), (M_AO, e1), (M_A2, jnp.logical_and(e1, jnp.logical_or(x >= 2, has_up))),
               (M_BT, jnp.logical_or(x_g > x, e2)), (M_BO, jnp.logical_or(x_f > x, e2)), (M_B2, jnp.logical_or(x < 2, has_up)),
               (M_P[PY1], e1), (M_P[PAT], e1), (M_P[PAO], e1), (M_P[PA2], e1), (M_P[PBT], e_bt), (M_P[PBO], e_bo),
               (M_P[PB2], e_b2), (M_P[PS], r_ps))
    part_sent = ((0, e1), (1, e1), (2, e1), (3, e1), (4, e_bt), (5, e_bo), (6, e_b2), (7, jnp.logical_or(core == 1, e2)),
                 (8 + R_DN, e_dn), (8 + R_2, e_x2), (8 + R_AT, e1), (8 + R_AO, e1), (8 + R_BT, e_bt), (8 + R_BO, e_bo),
                 (8 + R_Y2, e2), (8 + R_YA, e1))
    for j in range(2):
        for msg, e in kv_sent:
            pl.when(e)(lambda: kv_copy(msg, 0, 0, partner, j).wait_send())
    for q in range(4):
        for msg, e in part_sent:
            pl.when(e)(lambda: part_copy(msg, 0, dr.at[0, q], partner, q, 0).wait_send())
    o_out.wait()
    dq_out.wait()
    for c in outs:
        c.wait()


def emit_kernel(*refs):
    src, dst, buf, sem_in, sem_out = refs[:4], refs[4:8], refs[8:12], refs[12], refs[13]
    ins = [pltpu.make_async_copy(src[n], buf[n], sem_in.at[n]) for n in range(4)]
    outs = [pltpu.make_async_copy(buf[n], dst[n], sem_out.at[n]) for n in range(4)]
    for c in ins:
        c.start()
    for n in range(4):
        ins[n].wait()
        outs[n].start()
    for c in outs:
        c.wait()


def solution(mesh):
    seq_spec = P('dp', 'ctx', None, None)

    def local_attn(q_loc, k_loc, v_loc, do_loc):
        q = q_loc.reshape(NQ, HD)
        do = do_loc.reshape(NQ, HD)
        k = k_loc.reshape(CH, HD)
        v = v_loc.reshape(CH, HD)
        anyspec = pl.BlockSpec(memory_space=pl.ANY)
        o, dq, dk, dv = pl.pallas_call(
            kernel,
            out_shape=(jax.ShapeDtypeStruct((NQ, HD), BF16), jax.ShapeDtypeStruct((NQ, HD), BF16),
                       jax.ShapeDtypeStruct((CH, HD), BF16), jax.ShapeDtypeStruct((CH, HD), BF16)),
            in_specs=[anyspec] * 4,
            out_specs=[anyspec] * 4,
            scratch_shapes=[
                pltpu.VMEM((N_SLOT, 2, CH, HD), BF16),
                pltpu.VMEM((NQ, HD), BF16),
                pltpu.VMEM((NQ, HD), BF16),
                pltpu.VMEM((HD, NQ), BF16),
                pltpu.VMEM((HD, NQ), BF16),
                pltpu.VMEM((N_SLOT, CH, NQ), F32),
                pltpu.VMEM((N_SLOT, CH, NQ), F32),
                pltpu.VMEM((N_SLOT, 1, NQ), F32),
                pltpu.VMEM((1, NQ), F32),
                pltpu.VMEM((1, NQ), F32),
                pltpu.VMEM((1, NQ), F32),
                pltpu.VMEM((HD, NQ), F32),
                pltpu.VMEM((HD, NQ), F32),
                pltpu.VMEM((N_SLOT, 4, CH // 2, HD), F32),
                pltpu.VMEM((8, 4, CH // 2, HD), F32),
                pltpu.VMEM((8, 4, CH // 2, HD), F32),
                pltpu.VMEM((NQ, HD), BF16),
                pltpu.VMEM((NQ, HD), BF16),
                pltpu.VMEM((2, CH, HD), BF16),
                pltpu.VMEM((1, NQ), F32),
                pltpu.VMEM((CH, NQ), BF16),
                pltpu.SemaphoreType.DMA((8,)),
                pltpu.SemaphoreType.DMA((16, 2)),
                pltpu.SemaphoreType.DMA((N_SLOT, 2)),
                pltpu.SemaphoreType.DMA((16, 4)),
                pltpu.SemaphoreType.DMA((16, 4)),
            ],
            compiler_params=pltpu.CompilerParams(
                collective_id=0, has_side_effects=True, vmem_limit_bytes=63 * 1024 * 1024),
            name='swa_fwd_bwd',
        )(q, k, v, do)
        anyspec4 = [anyspec] * 4
        o, dq, dk, dv = pl.pallas_call(
            emit_kernel,
            out_shape=tuple(jax.ShapeDtypeStruct(a.shape, BF16) for a in (o, dq, dk, dv)),
            in_specs=anyspec4,
            out_specs=anyspec4,
            scratch_shapes=[pltpu.VMEM(a.shape, BF16) for a in (o, dq, dk, dv)] + [pltpu.SemaphoreType.DMA((4,))] * 2,
            name='emit',
        )(o, dq, dk, dv)
        return o.reshape(q_loc.shape), dq.reshape(q_loc.shape), dk.reshape(k_loc.shape), dv.reshape(k_loc.shape)

    return jax.shard_map(local_attn, mesh=mesh, in_specs=(seq_spec,) * 4, out_specs=(seq_spec,) * 4, check_vma=False)
```

```python
import functools

import jax
import jax.numpy as jnp
from jax import lax
from jax.experimental import pallas as pl
from jax.experimental.pallas import tpu as pltpu
from jax.sharding import PartitionSpec as P

OWN, Y1, AT, AO, A2, BT, BO, B2, Y2 = 0, 1, 3, 4, 7, 10, 11, 14, 16
PY1, PAT, PAO, PA2, PS, PBT, PBO, PB2 = 2, 5, 6, 8, 9, 12, 13, 15
N_SLOT = 17
ROW = 8
N_DEV = 128
CH = 256
NQ = 1024
HD = 128
TILE = 256
NEG_BIG = -1e30
LOG2E = 1.4426950408889634
SCALE = HD ** -0.5
F32 = jnp.float32
BF16 = jnp.bfloat16


def dot(a, b):
    return lax.dot_general(a, b, (((1,), (0,)), ((), ())), preferred_element_type=F32)


def kernel(q_hbm, k_hbm, v_hbm, do_hbm, o_hbm, dq_hbm, dk_hbm, dv_hbm,
           kv, q_s, do_s, qt_s, dot_s, p_buf, dp_buf, mh, m_s, l_s, d_s, ot_s, dqt_s, part,
           dr, rx, o_s, dq_s, dkv_s,
           al_s, pb_s, lsem, fs, fr, bs, br):
    me = lax.axis_index('ctx')
    core = lax.rem(me, 2)
    x = lax.rem(lax.div(me, 2), 4)
    odd = lax.rem(x, 2)
    base = me - 2 * x
    x_left = lax.rem(x + 3, 4)
    x_right = lax.rem(x + 1, 4)
    x_f = x_left + odd * (x_right - x_left)
    x_g = x_right + odd * (x_left - x_right)
    x_2 = lax.rem(x + 2, 4)
    dev_f = base + 2 * x_f
    dev_g = base + 2 * x_g
    dev_2 = base + 2 * x_2
    partner = me + 1 - 2 * core
    up = lax.rem(me + ROW, N_DEV)
    down = lax.rem(me + N_DEV - ROW, N_DEV)

    def dev(d):
        return {'dp': 0, 'ctx': d}

    loads = [
        pltpu.make_async_copy(k_hbm, kv.at[OWN, 0], lsem.at[0]),
        pltpu.make_async_copy(v_hbm, kv.at[OWN, 1], lsem.at[1]),
        pltpu.make_async_copy(q_hbm, q_s, lsem.at[2]),
        pltpu.make_async_copy(do_hbm, do_s, lsem.at[3]),
    ]
    for c in loads:
        c.start()

    row = lax.div(me, ROW)
    has_up = row < N_DEV // ROW - 1
    e1 = row >= 1
    e2 = row >= 2
    e_bt = jnp.logical_or(x_g < x, e2)
    e_bo = jnp.logical_or(x_f < x, e2)
    e_b2 = jnp.logical_or(x_2 < x, e2)

    barrier = pltpu.get_barrier_semaphore()

    def greet(d):
        pl.semaphore_signal(barrier, inc=1, device_id=dev(d), device_id_type=pl.DeviceIdType.MESH)

    pl.when(has_up)(lambda: greet(up))
    pl.when(e1)(lambda: greet(down))
    for d in (dev_f, dev_g, dev_2, partner):
        greet(d)
    pl.semaphore_wait(barrier, 4 + has_up.astype(jnp.int32) + e1.astype(jnp.int32))

    def kv_copy(msg, src, dst, d, j):
        return pltpu.make_async_remote_copy(
            src_ref=kv.at[src, j], dst_ref=kv.at[dst, j], send_sem=fs.at[msg, j], recv_sem=fr.at[dst, j],
            device_id=dev(d), device_id_type=pl.DeviceIdType.MESH)

    def kv_wait(slot, j):
        kv_copy(0, slot, slot, partner, j).wait_recv()

    def kv_send(msg, src, dst, d, j):
        kv_copy(msg, src, dst, d, j).start()

    M_Y1, M_Y2, M_AT, M_AO, M_A2, M_BT, M_BO, M_B2 = range(8)
    M_P = {PY1: 8, PAT: 9, PAO: 10, PA2: 11, PBT: 12, PBO: 13, PB2: 14, PS: 15}

    def to_partner(src, dst, j):
        kv_send(M_P[dst], src, dst, partner, j)

    for j in range(2):
        loads[j].wait()
        pl.when(has_up)(lambda: kv_send(M_Y1, OWN, Y1, up, j))
        pl.when(x_g > x)(lambda: kv_send(M_BT, OWN, BT, dev_g, j))
        pl.when(x_f > x)(lambda: kv_send(M_BO, OWN, BO, dev_f, j))
        pl.when(x_2 > x)(lambda: kv_send(M_B2, OWN, B2, dev_2, j))
        pl.when(core == 0)(lambda: to_partner(OWN, PS, j))

    loads[2].wait()
    loads[3].wait()
    for t in range(NQ // TILE):
        rows = pl.ds(t * TILE, TILE)
        qt_s[:, rows] = q_s[rows, :].T
        dot_s[:, rows] = do_s[rows, :].T
    m_s[...] = jnp.full_like(m_s, NEG_BIG)
    l_s[...] = jnp.zeros_like(l_s)
    ot_s[...] = jnp.zeros_like(ot_s)
    dqt_s[...] = jnp.zeros_like(dqt_s)

    def fwd_compute(slots, kind):
        vts = [kv[slot, 1].T for slot in slots]
        for t in range(NQ // TILE):
            ls = pl.ds(t * TILE, TILE)
            m = m_s[:, ls]
            for slot in slots:
                s = dot(kv[slot, 0], qt_s[:, ls])
                if kind is not None:
                    key = lax.broadcasted_iota(jnp.int32, (CH, TILE), 0)
                    tok = lax.shift_right_logical(lax.broadcasted_iota(jnp.int32, (CH, TILE), 1) + t * TILE, 2)
                    keep = key <= tok if kind == 'own' else key > tok
                    s = jnp.where(keep, s, NEG_BIG)
                p_buf[slot, :, ls] = s
                m = jnp.maximum(m, jnp.max(s, axis=0, keepdims=True) * (SCALE * LOG2E))
            for slot in slots:
                mh[slot, :, ls] = m
        for t in range(NQ // TILE):
            ls = pl.ds(t * TILE, TILE)
            m_new = mh[slots[0], :, ls]
            alpha = jnp.exp2(m_s[:, ls] - m_new)
            al_s[:, ls] = alpha
            m_s[:, ls] = m_new
            l = l_s[:, ls] * alpha
            for n, slot in enumerate(slots):
                p = jnp.exp2(p_buf[slot, :, ls] * (SCALE * LOG2E) - m_new)
                p_buf[slot, :, ls] = p
                dp_buf[slot, :, ls] = dot(kv[slot, 1], dot_s[:, ls])
                l = l + jnp.sum(p, axis=0, keepdims=True)
                pb_s[n, :, ls] = p.astype(BF16)
            l_s[:, ls] = l
        for t in range(NQ // TILE):
            ls = pl.ds(t * TILE, TILE)
            o = dot(vts[0], pb_s[0, :, ls])
            for n in range(1, len(slots)):
                o = o + dot(vts[n], pb_s[n, :, ls])
            ot_s[:, ls] = ot_s[:, ls] * al_s[:, ls] + o

    fwd_compute((OWN,), 'own')

    def here(i):
        def pick(c, u, v):
            return jnp.where(c, u.astype(jnp.int32), v)

        n = pick(i == OWN, row >= 0, pick(i <= PA2, e1, pick(i == PS, jnp.logical_or(core == 1, e2), pick(
            i == Y2, e2, pick(i >= B2, e_b2, pick(lax.rem(i, 2) == BT % 2, e_bt, e_bo.astype(jnp.int32)))))))
        return n > 0

    def take(slot, partner_slot, e):
        @pl.when(e)
        def _():
            for j in range(2):
                kv_wait(slot, j)
                to_partner(slot, partner_slot, j)

    def fwd_body(i, carry):
        @pl.when(jnp.logical_and(i == PY1, x >= 2))
        def _():
            for j in range(2):
                kv_wait(B2, j)
                pl.when(has_up)(lambda: kv_send(M_B2, B2, A2, up, j))
                to_partner(B2, PB2, j)


        @pl.when(here(i))
        def _():
            @pl.when(i == Y1)
            def _():
                for j in range(2):
                    kv_wait(Y1, j)
                    pl.when(has_up)(lambda: kv_send(M_Y2, Y1, Y2, up, j))
                    pl.when(x >= 2)(lambda: kv_send(M_A2, Y1, A2, dev_2, j))
                    kv_send(M_AT, Y1, AT, dev_f, j)
                    kv_send(M_AO, Y1, AO, dev_g, j)
                    to_partner(Y1, PY1, j)

            is_p = jnp.int32(0)
            for slot in M_P:
                is_p = is_p + (i == slot).astype(jnp.int32)

            @pl.when(is_p > 0)
            def _():
                kv_wait(i, 0)
                kv_wait(i, 1)

            fwd_compute((i,), None)

        return carry

    lax.fori_loop(1, AT, fwd_body, 0)

    @pl.when(e2)
    def _():
        kv_wait(Y2, 0)
        kv_wait(Y2, 1)
        fwd_compute((Y2,), 'far')

    def pair_body(k, carry):
        i = AT + 2 * k

        @pl.when(k == 0)
        def _():
            for j in range(2):
                @pl.when(x < 2)
                def _():
                    kv_wait(A2, j)
                    pl.when(has_up)(lambda: kv_send(M_A2, A2, B2, up, j))
                    to_partner(A2, PA2, j)

                kv_wait(AT, j)
                to_partner(AT, PAT, j)
                kv_wait(AO, j)
                to_partner(AO, PAO, j)

                @pl.when(e2)
                def _():
                    pl.when(x_g < x)(lambda: kv_send(M_BT, Y2, BT, dev_g, j))
                    pl.when(x_f < x)(lambda: kv_send(M_BO, Y2, BO, dev_f, j))
                    pl.when(core == 1)(lambda: to_partner(Y2, PS, j))

        @pl.when(k == 1)
        def _():
            @pl.when(x >= 2)
            def _():
                for j in range(2):
                    kv_wait(A2, j)
                    to_partner(A2, PA2, j)

            for j in range(2):
                kv_wait(PAT, j)
                kv_wait(PAO, j)

        @pl.when(k == 2)
        def _():
            for j in range(2):
                kv_wait(PA2, j)

        fwd_compute((i, i + 1), None)
        return carry

    @pl.when(e1)
    def _():
        lax.fori_loop(0, 3, pair_body, 0)

    take(BT, PBT, e_bt)
    take(BO, PBO, e_bo)
    lax.fori_loop(PS, PS + 1, fwd_body, 0)

    both = jnp.logical_and(e_b2, jnp.logical_and(e_bt, e_bo))

    def far_waits(k):
        for kk, pair in ((1, (PBT, PBO)), (2, (PB2,))):
            @pl.when(k == kk)
            def _(pair=pair):
                for slot in pair:
                    for j in range(2):
                        kv_wait(slot, j)

    def far_pairs(k, carry):
        @pl.when(k == 1)
        def _():
            take(B2, PB2, jnp.logical_and(x < 2, e2))

        far_waits(k)
        fwd_compute((BT + 2 * k, BT + 2 * k + 1), None)
        return carry

    @pl.when(both)
    def _():
        lax.fori_loop(0, 3, far_pairs, 0)

    @pl.when(jnp.logical_not(both))
    def _():
        lax.fori_loop(BT, N_SLOT - 1, fwd_body, 0)

    for t in range(NQ // TILE):
        ls = pl.ds(t * TILE, TILE)
        rl = 1.0 / l_s[:, ls]
        l_s[:, ls] = rl
        d_s[:, ls] = jnp.sum(ot_s[:, ls] * dot_s[:, ls].astype(F32), axis=0, keepdims=True) * rl

    def part_copy(msg, src, dst_ref, d, q, sem):
        return pltpu.make_async_remote_copy(
            src_ref=part.at[src, q], dst_ref=dst_ref, send_sem=bs.at[msg, q], recv_sem=br.at[sem, q],
            device_id=dev(d), device_id_type=pl.DeviceIdType.MESH)

    R_DN, R_2, R_AT, R_AO, R_BT, R_BO, R_Y2, R_YA = range(8)
    ORDER = (2, 3, 0, 1)

    def give(src, n):
        for q in ORDER:
            part_copy(n, src, dr.at[n, q], partner, q, n).start()

    def add_dr(slot, n, q):
        part_copy(n, 0, dr.at[n, q], partner, q, n).wait_recv()
        part[slot, q] += dr[n, q]

    def send(src, n, d, q):
        part_copy(8 + n, src, rx.at[n, q], d, q, 8 + n).start()

    def add_rx(slot, n, q):
        part_copy(8 + n, 0, rx.at[n, q], partner, q, 8 + n).wait_recv()
        part[slot, q] += rx[n, q]

    D_SLOT = {PY1: 0, PAT: 1, PAO: 2, PA2: 3, PBT: 4, PBO: 5, PB2: 6, PS: 7}

    def merge_send(slot, n_d, n_r, d):
        for q in ORDER:
            add_dr(slot, n_d, q)
            send(slot, n_r, d, q)

    hi = (x >= 2).astype(jnp.int32)
    low = x < 2
    s_dn, n_dn = B2 + hi * (A2 - B2), 6 - hi * 3
    s_x2, n_x2 = A2 + hi * (B2 - A2), 3 + hi * 3
    e_dn = jnp.logical_or(jnp.logical_and(low, e2), jnp.logical_and(x >= 2, e1))
    e_x2 = jnp.logical_or(x >= 2, e1)
    r_dn = jnp.logical_and(has_up, e_x2)

    B_ORDER = (PBT, PBO, PB2, PA2, BT, BO, B2, A2, PAT, PAO, PS, Y2, AT, AO, PY1, Y1, OWN)

    def bwd_compute(i):
        kb = kv[i, 0]
        kt = kb.T
        dk = jnp.zeros((CH, HD), F32)
        dv = jnp.zeros((CH, HD), F32)
        for t in range(NQ // TILE):
            ls = pl.ds(t * TILE, TILE)
            f = jnp.exp2(mh[i, :, ls] - m_s[:, ls]) * l_s[:, ls]
            p = p_buf[i, :, ls] * f
            dv = dv + dot(p.astype(BF16), do_s[ls, :])
            ds = (p * (dp_buf[i, :, ls] - d_s[:, ls])).astype(BF16)
            dk = dk + dot(ds, q_s[ls, :])
            dqt_s[:, ls] += dot(kt, ds)
        half = CH // 2
        part[i, 0] = dk[:half] * SCALE
        part[i, 1] = dk[half:] * SCALE
        part[i, 2] = dv[:half]
        part[i, 3] = dv[half:]

        for slot, n in D_SLOT.items():
            @pl.when(i == slot)
            def _(slot=slot, n=n):
                give(slot, n)

        @pl.when(i == BT)
        def _():
            merge_send(BT, 4, R_BT, dev_g)

        @pl.when(i == BO)
        def _():
            merge_send(BO, 5, R_BO, dev_f)

        @pl.when(i == AT)
        def _():
            merge_send(AT, 1, R_AT, dev_f)

        @pl.when(i == AO)
        def _():
            merge_send(AO, 2, R_AO, dev_g)

    def bwd_body(t0, carry):
        i = jnp.int32(0)
        for t, slot in enumerate(B_ORDER):
            i = jnp.where(t0 == t, slot, i)
        pl.when(here(i))(lambda: bwd_compute(i))

        @pl.when(jnp.logical_and(i == A2, e_dn))
        def _():
            merge_send(s_dn, n_dn, R_DN, down)

        return carry

    lax.fori_loop(0, N_SLOT, bwd_body, 0)

    def home_or_far(far):
        return far.astype(jnp.int32) * Y2

    r_bt = jnp.logical_or(x < x_g, e2)
    r_bo = jnp.logical_or(x < x_f, e2)
    r_ps = jnp.logical_or(core == 0, e2)

    def cross(q, e):
        @pl.when(e)
        def _():
            add_dr(s_x2, n_x2, q)
            pl.when(r_dn)(lambda: add_rx(s_x2, R_DN, q))
            send(s_x2, R_2, dev_2, q)

    def far(q):
        pl.when(r_ps)(lambda: add_dr(core * Y2, 7, q))
        pl.when(r_bt)(lambda: add_rx(home_or_far(x_g < x), R_BT, q))
        pl.when(r_bo)(lambda: add_rx(home_or_far(x_f < x), R_BO, q))
        pl.when(e2)(lambda: send(Y2, R_Y2, down, q))

    for t in range(NQ // TILE):
        ls = pl.ds(t * TILE, TILE)
        o_s[ls, :] = (ot_s[:, ls] * l_s[:, ls]).T.astype(BF16)
        dq_s[ls, :] = (dqt_s[:, ls] * SCALE).T.astype(BF16)
    o_out = pltpu.make_async_copy(o_s, o_hbm, lsem.at[4])
    o_out.start()
    dq_out = pltpu.make_async_copy(dq_s, dq_hbm, lsem.at[5])
    dq_out.start()

    for pair in ((2, 3), (0, 1)):
        for q in pair:
            far(q)
        for q in pair:
            cross(q, jnp.logical_and(low, e1))
    for q in ORDER:
        cross(q, x >= 2)
    for q in ORDER:
        @pl.when(e1)
        def _():
            add_dr(Y1, 0, q)
            add_rx(Y1, R_AT, q)
            add_rx(Y1, R_AO, q)
            pl.when(has_up)(lambda: add_rx(Y1, R_Y2, q))
            pl.when(x >= 2)(lambda: add_rx(Y1, R_2, q))
            send(Y1, R_YA, down, q)
    for q in ORDER:
        pl.when(low)(lambda: add_rx(OWN, R_2, q))
        pl.when(has_up)(lambda: add_rx(OWN, R_YA, q))
        dkv_s[q // 2, pl.ds(q % 2 * (CH // 2), CH // 2), :] = part[OWN, q].astype(BF16)
    outs = []
    for j, hbm in ((1, dv_hbm), (0, dk_hbm)):
        c = pltpu.make_async_copy(dkv_s.at[j], hbm, lsem.at[6 + j])
        c.start()
        outs.append(c)

    up1 = jnp.logical_and(has_up, e1)
    kv_sent = ((M_Y1, has_up), (M_Y2, up1), (M_AT, e1), (M_AO, e1), (M_A2, jnp.logical_and(e1, jnp.logical_or(x >= 2, has_up))),
               (M_BT, jnp.logical_or(x_g > x, e2)), (M_BO, jnp.logical_or(x_f > x, e2)), (M_B2, jnp.logical_or(x < 2, has_up)),
               (M_P[PY1], e1), (M_P[PAT], e1), (M_P[PAO], e1), (M_P[PA2], e1), (M_P[PBT], e_bt), (M_P[PBO], e_bo),
               (M_P[PB2], e_b2), (M_P[PS], r_ps))
    part_sent = ((0, e1), (1, e1), (2, e1), (3, e1), (4, e_bt), (5, e_bo), (6, e_b2), (7, jnp.logical_or(core == 1, e2)),
                 (8 + R_DN, e_dn), (8 + R_2, e_x2), (8 + R_AT, e1), (8 + R_AO, e1), (8 + R_BT, e_bt), (8 + R_BO, e_bo),
                 (8 + R_Y2, e2), (8 + R_YA, e1))
    for j in range(2):
        for msg, e in kv_sent:
            pl.when(e)(lambda: kv_copy(msg, 0, 0, partner, j).wait_send())
    for q in range(4):
        for msg, e in part_sent:
            pl.when(e)(lambda: part_copy(msg, 0, dr.at[0, q], partner, q, 0).wait_send())
    o_out.wait()
    dq_out.wait()
    for c in outs:
        c.wait()


def emit_kernel(*refs):
    src, dst, buf, sem_in, sem_out = refs[:4], refs[4:8], refs[8:12], refs[12], refs[13]
    ins = [pltpu.make_async_copy(src[n], buf[n], sem_in.at[n]) for n in range(4)]
    outs = [pltpu.make_async_copy(buf[n], dst[n], sem_out.at[n]) for n in range(4)]
    for c in ins:
        c.start()
    for n in range(4):
        ins[n].wait()
        outs[n].start()
    for c in outs:
        c.wait()


def solution(mesh):
    seq_spec = P('dp', 'ctx', None, None)

    def local_attn(q_loc, k_loc, v_loc, do_loc):
        q = q_loc.reshape(NQ, HD)
        do = do_loc.reshape(NQ, HD)
        k = k_loc.reshape(CH, HD)
        v = v_loc.reshape(CH, HD)
        anyspec = pl.BlockSpec(memory_space=pl.ANY)
        o, dq, dk, dv = pl.pallas_call(
            kernel,
            out_shape=(jax.ShapeDtypeStruct((NQ, HD), BF16), jax.ShapeDtypeStruct((NQ, HD), BF16),
                       jax.ShapeDtypeStruct((CH, HD), BF16), jax.ShapeDtypeStruct((CH, HD), BF16)),
            in_specs=[anyspec] * 4,
            out_specs=[anyspec] * 4,
            scratch_shapes=[
                pltpu.VMEM((N_SLOT, 2, CH, HD), BF16),
                pltpu.VMEM((NQ, HD), BF16),
                pltpu.VMEM((NQ, HD), BF16),
                pltpu.VMEM((HD, NQ), BF16),
                pltpu.VMEM((HD, NQ), BF16),
                pltpu.VMEM((N_SLOT, CH, NQ), F32),
                pltpu.VMEM((N_SLOT, CH, NQ), F32),
                pltpu.VMEM((N_SLOT, 1, NQ), F32),
                pltpu.VMEM((1, NQ), F32),
                pltpu.VMEM((1, NQ), F32),
                pltpu.VMEM((1, NQ), F32),
                pltpu.VMEM((HD, NQ), F32),
                pltpu.VMEM((HD, NQ), F32),
                pltpu.VMEM((N_SLOT, 4, CH // 2, HD), F32),
                pltpu.VMEM((8, 4, CH // 2, HD), F32),
                pltpu.VMEM((8, 4, CH // 2, HD), F32),
                pltpu.VMEM((NQ, HD), BF16),
                pltpu.VMEM((NQ, HD), BF16),
                pltpu.VMEM((2, CH, HD), BF16),
                pltpu.VMEM((1, NQ), F32),
                pltpu.VMEM((2, CH, NQ), BF16),
                pltpu.SemaphoreType.DMA((8,)),
                pltpu.SemaphoreType.DMA((16, 2)),
                pltpu.SemaphoreType.DMA((N_SLOT, 2)),
                pltpu.SemaphoreType.DMA((16, 4)),
                pltpu.SemaphoreType.DMA((16, 4)),
            ],
            compiler_params=pltpu.CompilerParams(
                collective_id=0, has_side_effects=True, vmem_limit_bytes=63 * 1024 * 1024),
            name='swa_fwd_bwd',
        )(q, k, v, do)
        anyspec4 = [anyspec] * 4
        o, dq, dk, dv = pl.pallas_call(
            emit_kernel,
            out_shape=tuple(jax.ShapeDtypeStruct(a.shape, BF16) for a in (o, dq, dk, dv)),
            in_specs=anyspec4,
            out_specs=anyspec4,
            scratch_shapes=[pltpu.VMEM(a.shape, BF16) for a in (o, dq, dk, dv)] + [pltpu.SemaphoreType.DMA((4,))] * 2,
            name='emit',
        )(o, dq, dk, dv)
        return o.reshape(q_loc.shape), dq.reshape(q_loc.shape), dk.reshape(k_loc.shape), dv.reshape(k_loc.shape)

    return jax.shard_map(local_attn, mesh=mesh, in_specs=(seq_spec,) * 4, out_specs=(seq_spec,) * 4, check_vma=False)
```

```python
import functools

import jax
import jax.numpy as jnp
from jax import lax
from jax.experimental import pallas as pl
from jax.experimental.pallas import tpu as pltpu
from jax.sharding import PartitionSpec as P

OWN, Y1, AT, AO, A2, BT, BO, B2, Y2 = 0, 1, 3, 4, 7, 10, 11, 14, 16
PY1, PAT, PAO, PA2, PS, PBT, PBO, PB2 = 2, 5, 6, 8, 9, 12, 13, 15
N_SLOT = 17
ROW = 8
N_DEV = 128
CH = 256
NQ = 1024
HD = 128
TILE = 256
NEG_BIG = -1e30
LOG2E = 1.4426950408889634
SCALE = HD ** -0.5
F32 = jnp.float32
BF16 = jnp.bfloat16


def dot(a, b):
    return lax.dot_general(a, b, (((1,), (0,)), ((), ())), preferred_element_type=F32)


def kernel(q_hbm, k_hbm, v_hbm, do_hbm, o_hbm, dq_hbm, dk_hbm, dv_hbm,
           kv, q_s, do_s, qt_s, dot_s, p_buf, dp_buf, mh, m_s, l_s, d_s, ot_s, dqt_s, part,
           dr, rx, o_s, dq_s, dkv_s,
           al_s, pb_s, lsem, fs, fr, bs, br):
    me = lax.axis_index('ctx')
    core = lax.rem(me, 2)
    x = lax.rem(lax.div(me, 2), 4)
    odd = lax.rem(x, 2)
    base = me - 2 * x
    x_left = lax.rem(x + 3, 4)
    x_right = lax.rem(x + 1, 4)
    x_f = x_left + odd * (x_right - x_left)
    x_g = x_right + odd * (x_left - x_right)
    x_2 = lax.rem(x + 2, 4)
    dev_f = base + 2 * x_f
    dev_g = base + 2 * x_g
    dev_2 = base + 2 * x_2
    partner = me + 1 - 2 * core
    up = lax.rem(me + ROW, N_DEV)
    down = lax.rem(me + N_DEV - ROW, N_DEV)

    def dev(d):
        return {'dp': 0, 'ctx': d}

    loads = [
        pltpu.make_async_copy(k_hbm, kv.at[OWN, 0], lsem.at[0]),
        pltpu.make_async_copy(v_hbm, kv.at[OWN, 1], lsem.at[1]),
        pltpu.make_async_copy(q_hbm, q_s, lsem.at[2]),
        pltpu.make_async_copy(do_hbm, do_s, lsem.at[3]),
    ]
    for c in loads:
        c.start()

    row = lax.div(me, ROW)
    has_up = row < N_DEV // ROW - 1
    e1 = row >= 1
    e2 = row >= 2
    e_bt = jnp.logical_or(x_g < x, e2)
    e_bo = jnp.logical_or(x_f < x, e2)
    e_b2 = jnp.logical_or(x_2 < x, e2)

    barrier = pltpu.get_barrier_semaphore()

    def greet(d):
        pl.semaphore_signal(barrier, inc=1, device_id=dev(d), device_id_type=pl.DeviceIdType.MESH)

    pl.when(has_up)(lambda: greet(up))
    pl.when(e1)(lambda: greet(down))
    for d in (dev_f, dev_g, dev_2, partner):
        greet(d)
    pl.semaphore_wait(barrier, 4 + has_up.astype(jnp.int32) + e1.astype(jnp.int32))

    def kv_copy(msg, src, dst, d, j):
        return pltpu.make_async_remote_copy(
            src_ref=kv.at[src, j], dst_ref=kv.at[dst, j], send_sem=fs.at[msg, j], recv_sem=fr.at[dst, j],
            device_id=dev(d), device_id_type=pl.DeviceIdType.MESH)

    def kv_wait(slot, j):
        kv_copy(0, slot, slot, partner, j).wait_recv()

    def kv_send(msg, src, dst, d, j):
        kv_copy(msg, src, dst, d, j).start()

    M_Y1, M_Y2, M_AT, M_AO, M_A2, M_BT, M_BO, M_B2 = range(8)
    M_P = {PY1: 8, PAT: 9, PAO: 10, PA2: 11, PBT: 12, PBO: 13, PB2: 14, PS: 15}

    def to_partner(src, dst, j):
        kv_send(M_P[dst], src, dst, partner, j)

    for j in range(2):
        loads[j].wait()
        pl.when(has_up)(lambda: kv_send(M_Y1, OWN, Y1, up, j))
        pl.when(x_g > x)(lambda: kv_send(M_BT, OWN, BT, dev_g, j))
        pl.when(x_f > x)(lambda: kv_send(M_BO, OWN, BO, dev_f, j))
        pl.when(x_2 > x)(lambda: kv_send(M_B2, OWN, B2, dev_2, j))
        pl.when(core == 0)(lambda: to_partner(OWN, PS, j))

    loads[2].wait()
    loads[3].wait()
    for t in range(NQ // TILE):
        rows = pl.ds(t * TILE, TILE)
        qt_s[:, rows] = q_s[rows, :].T
        dot_s[:, rows] = do_s[rows, :].T
    m_s[...] = jnp.full_like(m_s, NEG_BIG)
    l_s[...] = jnp.zeros_like(l_s)
    ot_s[...] = jnp.zeros_like(ot_s)
    dqt_s[...] = jnp.zeros_like(dqt_s)

    def fwd_compute(slots, kind):
        vts = [kv[slot, 1].T for slot in slots]
        for t in range(NQ // TILE):
            ls = pl.ds(t * TILE, TILE)
            m = m_s[:, ls]
            for slot in slots:
                s = dot(kv[slot, 0], qt_s[:, ls])
                if kind is not None:
                    key = lax.broadcasted_iota(jnp.int32, (CH, TILE), 0)
                    tok = lax.shift_right_logical(lax.broadcasted_iota(jnp.int32, (CH, TILE), 1) + t * TILE, 2)
                    keep = key <= tok if kind == 'own' else key > tok
                    s = jnp.where(keep, s, NEG_BIG)
                p_buf[slot, :, ls] = s
                m = jnp.maximum(m, jnp.max(s, axis=0, keepdims=True) * (SCALE * LOG2E))
            for slot in slots:
                mh[slot, :, ls] = m
        for t in range(NQ // TILE):
            ls = pl.ds(t * TILE, TILE)
            m_new = mh[slots[0], :, ls]
            alpha = jnp.exp2(m_s[:, ls] - m_new)
            al_s[:, ls] = alpha
            m_s[:, ls] = m_new
            l = l_s[:, ls] * alpha
            for n, slot in enumerate(slots):
                p = jnp.exp2(p_buf[slot, :, ls] * (SCALE * LOG2E) - m_new)
                p_buf[slot, :, ls] = p
                dp_buf[slot, :, ls] = dot(kv[slot, 1], dot_s[:, ls])
                l = l + jnp.sum(p, axis=0, keepdims=True)
                pb_s[n, :, ls] = p.astype(BF16)
            l_s[:, ls] = l
        for t in range(NQ // TILE):
            ls = pl.ds(t * TILE, TILE)
            o = dot(vts[0], pb_s[0, :, ls])
            for n in range(1, len(slots)):
                o = o + dot(vts[n], pb_s[n, :, ls])
            ot_s[:, ls] = ot_s[:, ls] * al_s[:, ls] + o

    fwd_compute((OWN,), 'own')

    def here(i):
        def pick(c, u, v):
            return jnp.where(c, u.astype(jnp.int32), v)

        n = pick(i == OWN, row >= 0, pick(i <= PA2, e1, pick(i == PS, jnp.logical_or(core == 1, e2), pick(
            i == Y2, e2, pick(i >= B2, e_b2, pick(lax.rem(i, 2) == BT % 2, e_bt, e_bo.astype(jnp.int32)))))))
        return n > 0

    def take(slot, partner_slot, e):
        @pl.when(e)
        def _():
            for j in range(2):
                kv_wait(slot, j)
                to_partner(slot, partner_slot, j)

    def fwd_body(i, carry):
        @pl.when(jnp.logical_and(i == PY1, x >= 2))
        def _():
            for j in range(2):
                kv_wait(B2, j)
                pl.when(has_up)(lambda: kv_send(M_B2, B2, A2, up, j))
                to_partner(B2, PB2, j)


        @pl.when(here(i))
        def _():
            @pl.when(i == Y1)
            def _():
                for j in range(2):
                    kv_wait(Y1, j)
                    pl.when(has_up)(lambda: kv_send(M_Y2, Y1, Y2, up, j))
                    pl.when(x >= 2)(lambda: kv_send(M_A2, Y1, A2, dev_2, j))
                    kv_send(M_AT, Y1, AT, dev_f, j)
                    kv_send(M_AO, Y1, AO, dev_g, j)
                    to_partner(Y1, PY1, j)

            is_p = jnp.int32(0)
            for slot in M_P:
                is_p = is_p + (i == slot).astype(jnp.int32)

            @pl.when(is_p > 0)
            def _():
                kv_wait(i, 0)
                kv_wait(i, 1)

            fwd_compute((i,), None)

        return carry

    lax.fori_loop(1, AT, fwd_body, 0)

    @pl.when(e2)
    def _():
        kv_wait(Y2, 0)
        kv_wait(Y2, 1)
        fwd_compute((Y2,), 'far')

    def pair_body(k, carry):
        i = AT + 2 * k

        @pl.when(k == 0)
        def _():
            for j in range(2):
                @pl.when(x < 2)
                def _():
                    kv_wait(A2, j)
                    pl.when(has_up)(lambda: kv_send(M_A2, A2, B2, up, j))
                    to_partner(A2, PA2, j)

                kv_wait(AT, j)
                to_partner(AT, PAT, j)
                kv_wait(AO, j)
                to_partner(AO, PAO, j)

                @pl.when(e2)
                def _():
                    pl.when(x_g < x)(lambda: kv_send(M_BT, Y2, BT, dev_g, j))
                    pl.when(x_f < x)(lambda: kv_send(M_BO, Y2, BO, dev_f, j))
                    pl.when(core == 1)(lambda: to_partner(Y2, PS, j))

        @pl.when(k == 1)
        def _():
            @pl.when(x >= 2)
            def _():
                for j in range(2):
                    kv_wait(A2, j)
                    to_partner(A2, PA2, j)

            for j in range(2):
                kv_wait(PAT, j)
                kv_wait(PAO, j)

        @pl.when(k == 2)
        def _():
            for j in range(2):
                kv_wait(PA2, j)

        fwd_compute((i, i + 1), None)
        return carry

    @pl.when(e1)
    def _():
        lax.fori_loop(0, 3, pair_body, 0)

    take(BT, PBT, e_bt)
    take(BO, PBO, e_bo)
    lax.fori_loop(PS, PS + 1, fwd_body, 0)

    both = jnp.logical_and(e_b2, jnp.logical_and(e_bt, e_bo))

    def far_waits(k):
        for kk, pair in ((1, (PBT, PBO)), (2, (PB2,))):
            @pl.when(k == kk)
            def _(pair=pair):
                for slot in pair:
                    for j in range(2):
                        kv_wait(slot, j)

    def far_pairs(k, carry):
        @pl.when(k == 1)
        def _():
            take(B2, PB2, jnp.logical_and(x < 2, e2))

        far_waits(k)
        fwd_compute((BT + 2 * k, BT + 2 * k + 1), None)
        return carry

    @pl.when(both)
    def _():
        lax.fori_loop(0, 3, far_pairs, 0)

    @pl.when(jnp.logical_not(both))
    def _():
        lax.fori_loop(BT, N_SLOT - 1, fwd_body, 0)

    for t in range(NQ // TILE):
        ls = pl.ds(t * TILE, TILE)
        rl = 1.0 / l_s[:, ls]
        l_s[:, ls] = rl
        d_s[:, ls] = jnp.sum(ot_s[:, ls] * dot_s[:, ls].astype(F32), axis=0, keepdims=True) * rl

    def part_copy(msg, src, dst_ref, d, q, sem):
        return pltpu.make_async_remote_copy(
            src_ref=part.at[src, q], dst_ref=dst_ref, send_sem=bs.at[msg, q], recv_sem=br.at[sem, q],
            device_id=dev(d), device_id_type=pl.DeviceIdType.MESH)

    R_DN, R_2, R_AT, R_AO, R_BT, R_BO, R_Y2, R_YA = range(8)
    ORDER = (2, 3, 0, 1)

    def give(src, n):
        for q in ORDER:
            part_copy(n, src, dr.at[n, q], partner, q, n).start()

    def add_dr(slot, n, q):
        part_copy(n, 0, dr.at[n, q], partner, q, n).wait_recv()
        part[slot, q] += dr[n, q]

    def send(src, n, d, q):
        part_copy(8 + n, src, rx.at[n, q], d, q, 8 + n).start()

    def add_rx(slot, n, q):
        part_copy(8 + n, 0, rx.at[n, q], partner, q, 8 + n).wait_recv()
        part[slot, q] += rx[n, q]

    D_SLOT = {PY1: 0, PAT: 1, PAO: 2, PA2: 3, PBT: 4, PBO: 5, PB2: 6, PS: 7}

    def merge_send(slot, n_d, n_r, d):
        for q in ORDER:
            add_dr(slot, n_d, q)
            send(slot, n_r, d, q)

    hi = (x >= 2).astype(jnp.int32)
    low = x < 2
    s_dn, n_dn = B2 + hi * (A2 - B2), 6 - hi * 3
    s_x2, n_x2 = A2 + hi * (B2 - A2), 3 + hi * 3
    e_dn = jnp.logical_or(jnp.logical_and(low, e2), jnp.logical_and(x >= 2, e1))
    e_x2 = jnp.logical_or(x >= 2, e1)
    r_dn = jnp.logical_and(has_up, e_x2)

    B_ORDER = (PBT, PBO, BT, BO, PB2, PA2, B2, A2, PAT, PAO, AT, AO, PS, Y2, PY1, Y1, OWN)

    def bwd_compute(i):
        kb = kv[i, 0]
        kt = kb.T
        dk = jnp.zeros((CH, HD), F32)
        dv = jnp.zeros((CH, HD), F32)
        for t in range(NQ // TILE):
            ls = pl.ds(t * TILE, TILE)
            f = jnp.exp2(mh[i, :, ls] - m_s[:, ls]) * l_s[:, ls]
            p = p_buf[i, :, ls] * f
            dv = dv + dot(p.astype(BF16), do_s[ls, :])
            ds = (p * (dp_buf[i, :, ls] - d_s[:, ls])).astype(BF16)
            dk = dk + dot(ds, q_s[ls, :])
            dqt_s[:, ls] += dot(kt, ds)
        half = CH // 2
        part[i, 0] = dk[:half] * SCALE
        part[i, 1] = dk[half:] * SCALE
        part[i, 2] = dv[:half]
        part[i, 3] = dv[half:]

        for slot, n in D_SLOT.items():
            @pl.when(i == slot)
            def _(slot=slot, n=n):
                give(slot, n)

        @pl.when(i == BT)
        def _():
            merge_send(BT, 4, R_BT, dev_g)

        @pl.when(i == BO)
        def _():
            merge_send(BO, 5, R_BO, dev_f)

        @pl.when(i == AT)
        def _():
            merge_send(AT, 1, R_AT, dev_f)

        @pl.when(i == AO)
        def _():
            merge_send(AO, 2, R_AO, dev_g)

    def bwd_body(t0, carry):
        i = jnp.int32(0)
        for t, slot in enumerate(B_ORDER):
            i = jnp.where(t0 == t, slot, i)
        pl.when(here(i))(lambda: bwd_compute(i))

        @pl.when(jnp.logical_and(i == A2, e_dn))
        def _():
            merge_send(s_dn, n_dn, R_DN, down)

        return carry

    lax.fori_loop(0, N_SLOT, bwd_body, 0)

    def home_or_far(far):
        return far.astype(jnp.int32) * Y2

    r_bt = jnp.logical_or(x < x_g, e2)
    r_bo = jnp.logical_or(x < x_f, e2)
    r_ps = jnp.logical_or(core == 0, e2)

    def cross(q, e):
        @pl.when(e)
        def _():
            add_dr(s_x2, n_x2, q)
            pl.when(r_dn)(lambda: add_rx(s_x2, R_DN, q))
            send(s_x2, R_2, dev_2, q)

    def far(q):
        pl.when(r_ps)(lambda: add_dr(core * Y2, 7, q))
        pl.when(r_bt)(lambda: add_rx(home_or_far(x_g < x), R_BT, q))
        pl.when(r_bo)(lambda: add_rx(home_or_far(x_f < x), R_BO, q))
        pl.when(e2)(lambda: send(Y2, R_Y2, down, q))

    for t in range(NQ // TILE):
        ls = pl.ds(t * TILE, TILE)
        o_s[ls, :] = (ot_s[:, ls] * l_s[:, ls]).T.astype(BF16)
        dq_s[ls, :] = (dqt_s[:, ls] * SCALE).T.astype(BF16)
    o_out = pltpu.make_async_copy(o_s, o_hbm, lsem.at[4])
    o_out.start()
    dq_out = pltpu.make_async_copy(dq_s, dq_hbm, lsem.at[5])
    dq_out.start()

    for pair in ((2, 3), (0, 1)):
        for q in pair:
            far(q)
        for q in pair:
            cross(q, jnp.logical_and(low, e1))
    for q in ORDER:
        cross(q, x >= 2)
    for q in ORDER:
        @pl.when(e1)
        def _():
            add_dr(Y1, 0, q)
            add_rx(Y1, R_AT, q)
            add_rx(Y1, R_AO, q)
            pl.when(has_up)(lambda: add_rx(Y1, R_Y2, q))
            pl.when(x >= 2)(lambda: add_rx(Y1, R_2, q))
            send(Y1, R_YA, down, q)
    for q in ORDER:
        pl.when(low)(lambda: add_rx(OWN, R_2, q))
        pl.when(has_up)(lambda: add_rx(OWN, R_YA, q))
        dkv_s[q // 2, pl.ds(q % 2 * (CH // 2), CH // 2), :] = part[OWN, q].astype(BF16)
    outs = []
    for j, hbm in ((1, dv_hbm), (0, dk_hbm)):
        c = pltpu.make_async_copy(dkv_s.at[j], hbm, lsem.at[6 + j])
        c.start()
        outs.append(c)

    up1 = jnp.logical_and(has_up, e1)
    kv_sent = ((M_Y1, has_up), (M_Y2, up1), (M_AT, e1), (M_AO, e1), (M_A2, jnp.logical_and(e1, jnp.logical_or(x >= 2, has_up))),
               (M_BT, jnp.logical_or(x_g > x, e2)), (M_BO, jnp.logical_or(x_f > x, e2)), (M_B2, jnp.logical_or(x < 2, has_up)),
               (M_P[PY1], e1), (M_P[PAT], e1), (M_P[PAO], e1), (M_P[PA2], e1), (M_P[PBT], e_bt), (M_P[PBO], e_bo),
               (M_P[PB2], e_b2), (M_P[PS], r_ps))
    part_sent = ((0, e1), (1, e1), (2, e1), (3, e1), (4, e_bt), (5, e_bo), (6, e_b2), (7, jnp.logical_or(core == 1, e2)),
                 (8 + R_DN, e_dn), (8 + R_2, e_x2), (8 + R_AT, e1), (8 + R_AO, e1), (8 + R_BT, e_bt), (8 + R_BO, e_bo),
                 (8 + R_Y2, e2), (8 + R_YA, e1))
    for j in range(2):
        for msg, e in kv_sent:
            pl.when(e)(lambda: kv_copy(msg, 0, 0, partner, j).wait_send())
    for q in range(4):
        for msg, e in part_sent:
            pl.when(e)(lambda: part_copy(msg, 0, dr.at[0, q], partner, q, 0).wait_send())
    o_out.wait()
    dq_out.wait()
    for c in outs:
        c.wait()


def emit_kernel(*refs):
    src, dst, buf, sem_in, sem_out = refs[:4], refs[4:8], refs[8:12], refs[12], refs[13]
    ins = [pltpu.make_async_copy(src[n], buf[n], sem_in.at[n]) for n in range(4)]
    outs = [pltpu.make_async_copy(buf[n], dst[n], sem_out.at[n]) for n in range(4)]
    for c in ins:
        c.start()
    for n in range(4):
        ins[n].wait()
        outs[n].start()
    for c in outs:
        c.wait()


def solution(mesh):
    seq_spec = P('dp', 'ctx', None, None)

    def local_attn(q_loc, k_loc, v_loc, do_loc):
        q = q_loc.reshape(NQ, HD)
        do = do_loc.reshape(NQ, HD)
        k = k_loc.reshape(CH, HD)
        v = v_loc.reshape(CH, HD)
        anyspec = pl.BlockSpec(memory_space=pl.ANY)
        o, dq, dk, dv = pl.pallas_call(
            kernel,
            out_shape=(jax.ShapeDtypeStruct((NQ, HD), BF16), jax.ShapeDtypeStruct((NQ, HD), BF16),
                       jax.ShapeDtypeStruct((CH, HD), BF16), jax.ShapeDtypeStruct((CH, HD), BF16)),
            in_specs=[anyspec] * 4,
            out_specs=[anyspec] * 4,
            scratch_shapes=[
                pltpu.VMEM((N_SLOT, 2, CH, HD), BF16),
                pltpu.VMEM((NQ, HD), BF16),
                pltpu.VMEM((NQ, HD), BF16),
                pltpu.VMEM((HD, NQ), BF16),
                pltpu.VMEM((HD, NQ), BF16),
                pltpu.VMEM((N_SLOT, CH, NQ), F32),
                pltpu.VMEM((N_SLOT, CH, NQ), F32),
                pltpu.VMEM((N_SLOT, 1, NQ), F32),
                pltpu.VMEM((1, NQ), F32),
                pltpu.VMEM((1, NQ), F32),
                pltpu.VMEM((1, NQ), F32),
                pltpu.VMEM((HD, NQ), F32),
                pltpu.VMEM((HD, NQ), F32),
                pltpu.VMEM((N_SLOT, 4, CH // 2, HD), F32),
                pltpu.VMEM((8, 4, CH // 2, HD), F32),
                pltpu.VMEM((8, 4, CH // 2, HD), F32),
                pltpu.VMEM((NQ, HD), BF16),
                pltpu.VMEM((NQ, HD), BF16),
                pltpu.VMEM((2, CH, HD), BF16),
                pltpu.VMEM((1, NQ), F32),
                pltpu.VMEM((2, CH, NQ), BF16),
                pltpu.SemaphoreType.DMA((8,)),
                pltpu.SemaphoreType.DMA((16, 2)),
                pltpu.SemaphoreType.DMA((N_SLOT, 2)),
                pltpu.SemaphoreType.DMA((16, 4)),
                pltpu.SemaphoreType.DMA((16, 4)),
            ],
            compiler_params=pltpu.CompilerParams(
                collective_id=0, has_side_effects=True, vmem_limit_bytes=63 * 1024 * 1024),
            name='swa_fwd_bwd',
        )(q, k, v, do)
        anyspec4 = [anyspec] * 4
        o, dq, dk, dv = pl.pallas_call(
            emit_kernel,
            out_shape=tuple(jax.ShapeDtypeStruct(a.shape, BF16) for a in (o, dq, dk, dv)),
            in_specs=anyspec4,
            out_specs=anyspec4,
            scratch_shapes=[pltpu.VMEM(a.shape, BF16) for a in (o, dq, dk, dv)] + [pltpu.SemaphoreType.DMA((4,))] * 2,
            name='emit',
        )(o, dq, dk, dv)
        return o.reshape(q_loc.shape), dq.reshape(q_loc.shape), dk.reshape(k_loc.shape), dv.reshape(k_loc.shape)

    return jax.shard_map(local_attn, mesh=mesh, in_specs=(seq_spec,) * 4, out_specs=(seq_spec,) * 4, check_vma=False)
```

```python
import functools

import jax
import jax.numpy as jnp
from jax import lax
from jax.experimental import pallas as pl
from jax.experimental.pallas import tpu as pltpu
from jax.sharding import PartitionSpec as P

OWN, Y1, AT, AO, A2, BT, BO, B2, Y2 = 0, 1, 3, 4, 7, 10, 11, 14, 16
PY1, PAT, PAO, PA2, PS, PBT, PBO, PB2 = 2, 5, 6, 8, 9, 12, 13, 15
N_SLOT = 17
ROW = 8
N_DEV = 128
CH = 256
NQ = 1024
HD = 128
TILE = 256
NEG_BIG = -1e30
LOG2E = 1.4426950408889634
SCALE = HD ** -0.5
F32 = jnp.float32
BF16 = jnp.bfloat16


def dot(a, b):
    return lax.dot_general(a, b, (((1,), (0,)), ((), ())), preferred_element_type=F32)


def kernel(q_hbm, k_hbm, v_hbm, do_hbm, o_hbm, dq_hbm, dk_hbm, dv_hbm,
           kv, q_s, do_s, qt_s, dot_s, p_buf, dp_buf, mh, m_s, l_s, d_s, ot_s, dqt_s, part,
           dr, rx, o_s, dq_s, dkv_s,
           al_s, pb_s, lsem, fs, fr, bs, br):
    me = lax.axis_index('ctx')
    core = lax.rem(me, 2)
    x = lax.rem(lax.div(me, 2), 4)
    odd = lax.rem(x, 2)
    base = me - 2 * x
    x_left = lax.rem(x + 3, 4)
    x_right = lax.rem(x + 1, 4)
    x_f = x_left + odd * (x_right - x_left)
    x_g = x_right + odd * (x_left - x_right)
    x_2 = lax.rem(x + 2, 4)
    dev_f = base + 2 * x_f
    dev_g = base + 2 * x_g
    dev_2 = base + 2 * x_2
    partner = me + 1 - 2 * core
    up = lax.rem(me + ROW, N_DEV)
    down = lax.rem(me + N_DEV - ROW, N_DEV)

    def dev(d):
        return {'dp': 0, 'ctx': d}

    loads = [
        pltpu.make_async_copy(k_hbm, kv.at[OWN, 0], lsem.at[0]),
        pltpu.make_async_copy(v_hbm, kv.at[OWN, 1], lsem.at[1]),
        pltpu.make_async_copy(q_hbm, q_s, lsem.at[2]),
        pltpu.make_async_copy(do_hbm, do_s, lsem.at[3]),
    ]
    for c in loads:
        c.start()

    row = lax.div(me, ROW)
    has_up = row < N_DEV // ROW - 1
    e1 = row >= 1
    e2 = row >= 2
    e_bt = jnp.logical_or(x_g < x, e2)
    e_bo = jnp.logical_or(x_f < x, e2)
    e_b2 = jnp.logical_or(x_2 < x, e2)

    barrier = pltpu.get_barrier_semaphore()

    def greet(d):
        pl.semaphore_signal(barrier, inc=1, device_id=dev(d), device_id_type=pl.DeviceIdType.MESH)

    pl.when(has_up)(lambda: greet(up))
    pl.when(e1)(lambda: greet(down))
    for d in (dev_f, dev_g, dev_2, partner):
        greet(d)
    pl.semaphore_wait(barrier, 4 + has_up.astype(jnp.int32) + e1.astype(jnp.int32))

    def kv_copy(msg, src, dst, d, j):
        return pltpu.make_async_remote_copy(
            src_ref=kv.at[src, j], dst_ref=kv.at[dst, j], send_sem=fs.at[msg, j], recv_sem=fr.at[dst, j],
            device_id=dev(d), device_id_type=pl.DeviceIdType.MESH)

    def kv_wait(slot, j):
        kv_copy(0, slot, slot, partner, j).wait_recv()

    def kv_send(msg, src, dst, d, j):
        kv_copy(msg, src, dst, d, j).start()

    M_Y1, M_Y2, M_AT, M_AO, M_A2, M_BT, M_BO, M_B2 = range(8)
    M_P = {PY1: 8, PAT: 9, PAO: 10, PA2: 11, PBT: 12, PBO: 13, PB2: 14, PS: 15}

    def to_partner(src, dst, j):
        kv_send(M_P[dst], src, dst, partner, j)

    for j in range(2):
        loads[j].wait()
        pl.when(has_up)(lambda: kv_send(M_Y1, OWN, Y1, up, j))
        pl.when(x_g > x)(lambda: kv_send(M_BT, OWN, BT, dev_g, j))
        pl.when(x_f > x)(lambda: kv_send(M_BO, OWN, BO, dev_f, j))
        pl.when(x_2 > x)(lambda: kv_send(M_B2, OWN, B2, dev_2, j))
        pl.when(core == 0)(lambda: to_partner(OWN, PS, j))

    loads[2].wait()
    loads[3].wait()
    for t in range(NQ // TILE):
        rows = pl.ds(t * TILE, TILE)
        qt_s[:, rows] = q_s[rows, :].T
        dot_s[:, rows] = do_s[rows, :].T
    m_s[...] = jnp.full_like(m_s, NEG_BIG)
    l_s[...] = jnp.zeros_like(l_s)
    ot_s[...] = jnp.zeros_like(ot_s)
    dqt_s[...] = jnp.zeros_like(dqt_s)

    def fwd_compute(slots, kind):
        vts = [kv[slot, 1].T for slot in slots]
        for t in range(NQ // TILE):
            ls = pl.ds(t * TILE, TILE)
            m = m_s[:, ls]
            for slot in slots:
                s = dot(kv[slot, 0], qt_s[:, ls])
                if kind is not None:
                    key = lax.broadcasted_iota(jnp.int32, (CH, TILE), 0)
                    tok = lax.shift_right_logical(lax.broadcasted_iota(jnp.int32, (CH, TILE), 1) + t * TILE, 2)
                    keep = key <= tok if kind == 'own' else key > tok
                    s = jnp.where(keep, s, NEG_BIG)
                p_buf[slot, :, ls] = s
                m = jnp.maximum(m, jnp.max(s, axis=0, keepdims=True) * (SCALE * LOG2E))
            for slot in slots:
                mh[slot, :, ls] = m
        for t in range(NQ // TILE):
            ls = pl.ds(t * TILE, TILE)
            m_new = mh[slots[0], :, ls]
            alpha = jnp.exp2(m_s[:, ls] - m_new)
            al_s[:, ls] = alpha
            m_s[:, ls] = m_new
            l = l_s[:, ls] * alpha
            for n, slot in enumerate(slots):
                p = jnp.exp2(p_buf[slot, :, ls] * (SCALE * LOG2E) - m_new)
                p_buf[slot, :, ls] = p
                dp_buf[slot, :, ls] = dot(kv[slot, 1], dot_s[:, ls])
                l = l + jnp.sum(p, axis=0, keepdims=True)
                pb_s[n, :, ls] = p.astype(BF16)
            l_s[:, ls] = l
        for t in range(NQ // TILE):
            ls = pl.ds(t * TILE, TILE)
            o = dot(vts[0], pb_s[0, :, ls])
            for n in range(1, len(slots)):
                o = o + dot(vts[n], pb_s[n, :, ls])
            ot_s[:, ls] = ot_s[:, ls] * al_s[:, ls] + o

    fwd_compute((OWN,), 'own')

    def here(i):
        def pick(c, u, v):
            return jnp.where(c, u.astype(jnp.int32), v)

        n = pick(i == OWN, row >= 0, pick(i <= PA2, e1, pick(i == PS, jnp.logical_or(core == 1, e2), pick(
            i == Y2, e2, pick(i >= B2, e_b2, pick(lax.rem(i, 2) == BT % 2, e_bt, e_bo.astype(jnp.int32)))))))
        return n > 0

    def take(slot, partner_slot, e):
        @pl.when(e)
        def _():
            for j in range(2):
                kv_wait(slot, j)
                to_partner(slot, partner_slot, j)

    def fwd_body(i, carry):
        @pl.when(jnp.logical_and(i == PY1, x >= 2))
        def _():
            for j in range(2):
                kv_wait(B2, j)
                pl.when(has_up)(lambda: kv_send(M_B2, B2, A2, up, j))
                to_partner(B2, PB2, j)


        @pl.when(here(i))
        def _():
            @pl.when(i == Y1)
            def _():
                for j in range(2):
                    kv_wait(Y1, j)
                    pl.when(has_up)(lambda: kv_send(M_Y2, Y1, Y2, up, j))
                    pl.when(x >= 2)(lambda: kv_send(M_A2, Y1, A2, dev_2, j))
                    kv_send(M_AT, Y1, AT, dev_f, j)
                    kv_send(M_AO, Y1, AO, dev_g, j)
                    to_partner(Y1, PY1, j)

            is_p = jnp.int32(0)
            for slot in M_P:
                is_p = is_p + (i == slot).astype(jnp.int32)

            @pl.when(is_p > 0)
            def _():
                kv_wait(i, 0)
                kv_wait(i, 1)

            fwd_compute((i,), None)

        return carry

    lax.fori_loop(1, AT, fwd_body, 0)

    @pl.when(e2)
    def _():
        kv_wait(Y2, 0)
        kv_wait(Y2, 1)
        fwd_compute((Y2,), 'far')

    def pair_body(k, carry):
        i = AT + 2 * k

        @pl.when(k == 0)
        def _():
            for j in range(2):
                @pl.when(x < 2)
                def _():
                    kv_wait(A2, j)
                    pl.when(has_up)(lambda: kv_send(M_A2, A2, B2, up, j))
                    to_partner(A2, PA2, j)

                kv_wait(AT, j)
                to_partner(AT, PAT, j)
                kv_wait(AO, j)
                to_partner(AO, PAO, j)

                @pl.when(e2)
                def _():
                    pl.when(x_g < x)(lambda: kv_send(M_BT, Y2, BT, dev_g, j))
                    pl.when(x_f < x)(lambda: kv_send(M_BO, Y2, BO, dev_f, j))
                    pl.when(core == 1)(lambda: to_partner(Y2, PS, j))

        @pl.when(k == 1)
        def _():
            @pl.when(x >= 2)
            def _():
                for j in range(2):
                    kv_wait(A2, j)
                    to_partner(A2, PA2, j)

            for j in range(2):
                kv_wait(PAT, j)
                kv_wait(PAO, j)

        @pl.when(k == 2)
        def _():
            for j in range(2):
                kv_wait(PA2, j)

        fwd_compute((i, i + 1), None)
        return carry

    @pl.when(e1)
    def _():
        lax.fori_loop(0, 3, pair_body, 0)

    take(BT, PBT, e_bt)
    take(BO, PBO, e_bo)
    lax.fori_loop(PS, PS + 1, fwd_body, 0)

    both = jnp.logical_and(e_b2, jnp.logical_and(e_bt, e_bo))

    def far_waits(k):
        for kk, pair in ((1, (PBT, PBO)), (2, (PB2,))):
            @pl.when(k == kk)
            def _(pair=pair):
                for slot in pair:
                    for j in range(2):
                        kv_wait(slot, j)

    def far_pairs(k, carry):
        @pl.when(k == 1)
        def _():
            take(B2, PB2, jnp.logical_and(x < 2, e2))

        far_waits(k)
        fwd_compute((BT + 2 * k, BT + 2 * k + 1), None)
        return carry

    @pl.when(both)
    def _():
        lax.fori_loop(0, 3, far_pairs, 0)

    @pl.when(jnp.logical_not(both))
    def _():
        lax.fori_loop(BT, N_SLOT - 1, fwd_body, 0)

    for t in range(NQ // TILE):
        ls = pl.ds(t * TILE, TILE)
        rl = 1.0 / l_s[:, ls]
        l_s[:, ls] = rl
        d_s[:, ls] = jnp.sum(ot_s[:, ls] * dot_s[:, ls].astype(F32), axis=0, keepdims=True) * rl

    def part_copy(msg, src, dst_ref, d, q, sem):
        return pltpu.make_async_remote_copy(
            src_ref=part.at[src, q], dst_ref=dst_ref, send_sem=bs.at[msg, q], recv_sem=br.at[sem, q],
            device_id=dev(d), device_id_type=pl.DeviceIdType.MESH)

    R_DN, R_2, R_AT, R_AO, R_BT, R_BO, R_Y2, R_YA = range(8)
    ORDER = (2, 3, 0, 1)

    def give(src, n):
        for q in ORDER:
            part_copy(n, src, dr.at[n, q], partner, q, n).start()

    def add_dr(slot, n, q):
        part_copy(n, 0, dr.at[n, q], partner, q, n).wait_recv()
        part[slot, q] += dr[n, q]

    def send(src, n, d, q):
        part_copy(8 + n, src, rx.at[n, q], d, q, 8 + n).start()

    def add_rx(slot, n, q):
        part_copy(8 + n, 0, rx.at[n, q], partner, q, 8 + n).wait_recv()
        part[slot, q] += rx[n, q]

    D_SLOT = {PY1: 0, PAT: 1, PAO: 2, PA2: 3, PBT: 4, PBO: 5, PB2: 6, PS: 7}

    def merge_send(slot, n_d, n_r, d):
        for q in ORDER:
            add_dr(slot, n_d, q)
            send(slot, n_r, d, q)

    hi = (x >= 2).astype(jnp.int32)
    low = x < 2
    s_dn, n_dn = B2 + hi * (A2 - B2), 6 - hi * 3
    s_x2, n_x2 = A2 + hi * (B2 - A2), 3 + hi * 3
    e_dn = jnp.logical_or(jnp.logical_and(low, e2), jnp.logical_and(x >= 2, e1))
    e_x2 = jnp.logical_or(x >= 2, e1)
    r_dn = jnp.logical_and(has_up, e_x2)

    B_ORDER = (PBT, PBO, BT, BO, PB2, PA2, B2, A2, PAT, PAO, AT, AO, PS, Y2, PY1, Y1, OWN)

    def bwd_compute(i):
        kb = kv[i, 0]
        kt = kb.T
        dk = jnp.zeros((CH, HD), F32)
        dv = jnp.zeros((CH, HD), F32)
        for t in range(NQ // TILE):
            ls = pl.ds(t * TILE, TILE)
            f = jnp.exp2(mh[i, :, ls] - m_s[:, ls]) * l_s[:, ls]
            p = p_buf[i, :, ls] * f
            dv = dv + dot(p.astype(BF16), do_s[ls, :])
            ds = (p * (dp_buf[i, :, ls] - d_s[:, ls])).astype(BF16)
            dk = dk + dot(ds, q_s[ls, :])
            dqt_s[:, ls] += dot(kt, ds)
        half = CH // 2
        part[i, 0] = dk[:half] * SCALE
        part[i, 1] = dk[half:] * SCALE
        part[i, 2] = dv[:half]
        part[i, 3] = dv[half:]

        for slot, n in D_SLOT.items():
            @pl.when(i == slot)
            def _(slot=slot, n=n):
                give(slot, n)

        @pl.when(i == BT)
        def _():
            merge_send(BT, 4, R_BT, dev_g)

        @pl.when(i == BO)
        def _():
            merge_send(BO, 5, R_BO, dev_f)

        @pl.when(i == AT)
        def _():
            merge_send(AT, 1, R_AT, dev_f)

        @pl.when(i == AO)
        def _():
            merge_send(AO, 2, R_AO, dev_g)

    def bwd_body(t0, carry):
        i = jnp.int32(0)
        for t, slot in enumerate(B_ORDER):
            i = jnp.where(t0 == t, slot, i)
        pl.when(here(i))(lambda: bwd_compute(i))

        @pl.when(jnp.logical_and(i == A2, e_dn))
        def _():
            merge_send(s_dn, n_dn, R_DN, down)

        return carry

    lax.fori_loop(0, N_SLOT, bwd_body, 0)

    def home_or_far(far):
        return far.astype(jnp.int32) * Y2

    r_bt = jnp.logical_or(x < x_g, e2)
    r_bo = jnp.logical_or(x < x_f, e2)
    r_ps = jnp.logical_or(core == 0, e2)

    def cross(q, e):
        @pl.when(e)
        def _():
            add_dr(s_x2, n_x2, q)
            pl.when(r_dn)(lambda: add_rx(s_x2, R_DN, q))
            send(s_x2, R_2, dev_2, q)

    def far(q):
        pl.when(r_ps)(lambda: add_dr(core * Y2, 7, q))
        pl.when(r_bt)(lambda: add_rx(home_or_far(x_g < x), R_BT, q))
        pl.when(r_bo)(lambda: add_rx(home_or_far(x_f < x), R_BO, q))
        pl.when(e2)(lambda: send(Y2, R_Y2, down, q))

    for pair in ((2, 3), (0, 1)):
        for q in pair:
            far(q)
        for q in pair:
            cross(q, jnp.logical_and(low, e1))
    for q in ORDER:
        cross(q, x >= 2)

    for t in range(NQ // TILE):
        ls = pl.ds(t * TILE, TILE)
        o_s[ls, :] = (ot_s[:, ls] * l_s[:, ls]).T.astype(BF16)
        dq_s[ls, :] = (dqt_s[:, ls] * SCALE).T.astype(BF16)
    o_out = pltpu.make_async_copy(o_s, o_hbm, lsem.at[4])
    o_out.start()
    dq_out = pltpu.make_async_copy(dq_s, dq_hbm, lsem.at[5])
    dq_out.start()

    for q in ORDER:
        @pl.when(e1)
        def _():
            add_dr(Y1, 0, q)
            add_rx(Y1, R_AT, q)
            add_rx(Y1, R_AO, q)
            pl.when(has_up)(lambda: add_rx(Y1, R_Y2, q))
            pl.when(x >= 2)(lambda: add_rx(Y1, R_2, q))
            send(Y1, R_YA, down, q)
    outs = []
    for j, hbm in ((1, dv_hbm), (0, dk_hbm)):
        for q in (2 * j, 2 * j + 1):
            pl.when(low)(lambda: add_rx(OWN, R_2, q))
            pl.when(has_up)(lambda: add_rx(OWN, R_YA, q))
            dkv_s[j, pl.ds(q % 2 * (CH // 2), CH // 2), :] = part[OWN, q].astype(BF16)
        c = pltpu.make_async_copy(dkv_s.at[j], hbm, lsem.at[6 + j])
        c.start()
        outs.append(c)

    up1 = jnp.logical_and(has_up, e1)
    kv_sent = ((M_Y1, has_up), (M_Y2, up1), (M_AT, e1), (M_AO, e1), (M_A2, jnp.logical_and(e1, jnp.logical_or(x >= 2, has_up))),
               (M_BT, jnp.logical_or(x_g > x, e2)), (M_BO, jnp.logical_or(x_f > x, e2)), (M_B2, jnp.logical_or(x < 2, has_up)),
               (M_P[PY1], e1), (M_P[PAT], e1), (M_P[PAO], e1), (M_P[PA2], e1), (M_P[PBT], e_bt), (M_P[PBO], e_bo),
               (M_P[PB2], e_b2), (M_P[PS], r_ps))
    part_sent = ((0, e1), (1, e1), (2, e1), (3, e1), (4, e_bt), (5, e_bo), (6, e_b2), (7, jnp.logical_or(core == 1, e2)),
                 (8 + R_DN, e_dn), (8 + R_2, e_x2), (8 + R_AT, e1), (8 + R_AO, e1), (8 + R_BT, e_bt), (8 + R_BO, e_bo),
                 (8 + R_Y2, e2), (8 + R_YA, e1))
    for j in range(2):
        for msg, e in kv_sent:
            pl.when(e)(lambda: kv_copy(msg, 0, 0, partner, j).wait_send())
    for q in range(4):
        for msg, e in part_sent:
            pl.when(e)(lambda: part_copy(msg, 0, dr.at[0, q], partner, q, 0).wait_send())
    o_out.wait()
    dq_out.wait()
    for c in outs:
        c.wait()


def emit_kernel(*refs):
    src, dst, buf, sem_in, sem_out = refs[:4], refs[4:8], refs[8:12], refs[12], refs[13]
    ins = [pltpu.make_async_copy(src[n], buf[n], sem_in.at[n]) for n in range(4)]
    outs = [pltpu.make_async_copy(buf[n], dst[n], sem_out.at[n]) for n in range(4)]
    for c in ins:
        c.start()
    for n in range(4):
        ins[n].wait()
        outs[n].start()
    for c in outs:
        c.wait()


def solution(mesh):
    seq_spec = P('dp', 'ctx', None, None)

    def local_attn(q_loc, k_loc, v_loc, do_loc):
        q = q_loc.reshape(NQ, HD)
        do = do_loc.reshape(NQ, HD)
        k = k_loc.reshape(CH, HD)
        v = v_loc.reshape(CH, HD)
        anyspec = pl.BlockSpec(memory_space=pl.ANY)
        o, dq, dk, dv = pl.pallas_call(
            kernel,
            out_shape=(jax.ShapeDtypeStruct((NQ, HD), BF16), jax.ShapeDtypeStruct((NQ, HD), BF16),
                       jax.ShapeDtypeStruct((CH, HD), BF16), jax.ShapeDtypeStruct((CH, HD), BF16)),
            in_specs=[anyspec] * 4,
            out_specs=[anyspec] * 4,
            scratch_shapes=[
                pltpu.VMEM((N_SLOT, 2, CH, HD), BF16),
                pltpu.VMEM((NQ, HD), BF16),
                pltpu.VMEM((NQ, HD), BF16),
                pltpu.VMEM((HD, NQ), BF16),
                pltpu.VMEM((HD, NQ), BF16),
                pltpu.VMEM((N_SLOT, CH, NQ), F32),
                pltpu.VMEM((N_SLOT, CH, NQ), F32),
                pltpu.VMEM((N_SLOT, 1, NQ), F32),
                pltpu.VMEM((1, NQ), F32),
                pltpu.VMEM((1, NQ), F32),
                pltpu.VMEM((1, NQ), F32),
                pltpu.VMEM((HD, NQ), F32),
                pltpu.VMEM((HD, NQ), F32),
                pltpu.VMEM((N_SLOT, 4, CH // 2, HD), F32),
                pltpu.VMEM((8, 4, CH // 2, HD), F32),
                pltpu.VMEM((8, 4, CH // 2, HD), F32),
                pltpu.VMEM((NQ, HD), BF16),
                pltpu.VMEM((NQ, HD), BF16),
                pltpu.VMEM((2, CH, HD), BF16),
                pltpu.VMEM((1, NQ), F32),
                pltpu.VMEM((2, CH, NQ), BF16),
                pltpu.SemaphoreType.DMA((8,)),
                pltpu.SemaphoreType.DMA((16, 2)),
                pltpu.SemaphoreType.DMA((N_SLOT, 2)),
                pltpu.SemaphoreType.DMA((16, 4)),
                pltpu.SemaphoreType.DMA((16, 4)),
            ],
            compiler_params=pltpu.CompilerParams(
                collective_id=0, has_side_effects=True, vmem_limit_bytes=63 * 1024 * 1024),
            name='swa_fwd_bwd',
        )(q, k, v, do)
        anyspec4 = [anyspec] * 4
        o, dq, dk, dv = pl.pallas_call(
            emit_kernel,
            out_shape=tuple(jax.ShapeDtypeStruct(a.shape, BF16) for a in (o, dq, dk, dv)),
            in_specs=anyspec4,
            out_specs=anyspec4,
            scratch_shapes=[pltpu.VMEM(a.shape, BF16) for a in (o, dq, dk, dv)] + [pltpu.SemaphoreType.DMA((4,))] * 2,
            name='emit',
        )(o, dq, dk, dv)
        return o.reshape(q_loc.shape), dq.reshape(q_loc.shape), dk.reshape(k_loc.shape), dv.reshape(k_loc.shape)

    return jax.shard_map(local_attn, mesh=mesh, in_specs=(seq_spec,) * 4, out_specs=(seq_spec,) * 4, check_vma=False)
```
